32 devices in a mesh: client: 32 (over z, y, x, core).
Axes of the slice: x: 2, y: 2, z: 4, core: 2. Of those that a mesh axis runs over, the one named last changes fastest.
Arguments:
- patches: bfloat16 [4096, 192], P('client'), may hold values from -6 to 6
- labels: int32 [256], replicated, may hold values from 0 to 9
- assign: int32 [32, 1], replicated, may hold values from 0 to 15; in each aligned block of 32 rows (0 to 31, 32 to 63, ...) at most 4 rows name the same one
- patch_embed: bfloat16 [192, 384], replicated, may hold values from -0.4375 to 0.4375
- positions: bfloat16 [16, 384], replicated, may hold values from -3 to 3
- client_in: bfloat16 [384, 3072], replicated, may hold values from -3 to 3
- client_down: bfloat16 [1536, 384], replicated, may hold values from -0.15625 to 0.15625
- server_in: bfloat16 [2, 6144, 3072], P(None, 'client'), may hold values from -3 to 3
- server_down: bfloat16 [2, 24576, 384], P(None, 'client'), may hold values from -0.15625 to 0.15625
- classifier: bfloat16 [16, 384, 10], replicated, may hold values from -15 to 15
Outputs:
- losses: float32 [32, 16], P('client')
- grad_patch_embed: float32 [192, 384], P(None, 'client')
- grad_positions: float32 [16, 384], P(None, 'client')
- grad_client_in: float32 [384, 3072], P(None, 'client')
- grad_client_down: float32 [1536, 384], P(None, 'client')
- grad_server_in: float32 [2, 6144, 3072], P(None, 'client')
- grad_server_down: float32 [2, 24576, 384], P(None, 'client')
- grad_classifier: float32 [6144, 10], P('client')
The draws below stay inside these ranges and needn't reach their ends.
Inputs may be any that keep to these rules, and one draw needn't show every extreme that they name: `assign`: no server shard is named by more than 4 clients, a bound that some block reaches.
All inputs are finite; a program needn't handle non-finite values.
Results may differ from the reference program's by a relative error of at most 0.025.
Values may be sent and summed in bfloat16 or wider, within the bound.
A program may use at most 128 MiB of HBM per device.

```python
import math
import jax
import jax.numpy as jnp
import numpy as np
from jax import lax

D = 384
HEADS = 6
FF = 1536
PATCH = 192
TOK = 16
CLASSES = 10
IMG = 8
SHARDS = 16
SLOTS = 2
SERVER_LAYERS = 2
CAPACITY = 4
N_CLIENT = 32


def scaled_normal(key, shape, fan_in):
    return jax.random.truncated_normal(key, -4.0, 4.0, shape, jnp.float32) / math.sqrt(fan_in)


def draw_client_in(key, part):
    values = scaled_normal(jax.random.fold_in(key, 11), (D, 4 * D + FF), D)
    return values.astype(jnp.bfloat16)


def draw_server_in(key, part):
    values = scaled_normal(jax.random.fold_in(key, 23), (SERVER_LAYERS, SHARDS * D, 4 * D + FF), D)
    return values.astype(jnp.bfloat16)


def draw_classifier(key, part):
    values = scaled_normal(jax.random.fold_in(key, 37), (SHARDS, D, CLASSES), D)
    return values.astype(jnp.bfloat16)


def place_ends(result, key, least, high):
    dims = result.shape
    place = [jax.random.randint(jax.random.fold_in(key, axis), (), 0, dims[axis]) for axis in range(len(dims))]
    result = result.at[tuple(place)].set(least)
    longest = dims.index(max(dims))
    place[longest] = (place[longest] + 1) % dims[longest]
    return result.at[tuple(place)].set(high)


def levels(key, extent, split, least, top_value):
    level, own = 1.0, jax.random.fold_in(key, 6)
    for dim, blocks in split:
        steps = jnp.exp(jax.random.uniform(jax.random.fold_in(own, dim), (blocks,), jnp.float32, least / len(split), top_value / len(split)))
        level = level * jnp.repeat(steps, extent[dim] // blocks).reshape([-1 if axis == dim else 1 for axis in range(len(extent))])
    return level


def assign_block(stream_key, own, number, rows, amount, top, reach, lean):
    sequence = jax.random.permutation(stream_key, amount)
    heavy_load, common = shares(amount, rows * top, reach, lean, True), shares(amount, rows * top, reach, lean, False)
    places = jnp.arange(amount)

    def named(sizes, rotation):
        used = int((sizes > 0).sum())
        fixed = max(1, used // 4)
        shifted = fixed + (places - fixed + rotation * (used - fixed)) % max(1, amount - fixed)
        return jnp.zeros((amount,), jnp.int32).at[sequence[jnp.where(places < fixed, places, shifted)]].set(jnp.asarray(sizes, jnp.int32))

    sizes = jnp.where(number % 4 == 0, named(heavy_load, number // 4), named(common, number - number // 4 - 1))
    mixed = jax.random.permutation(jax.random.fold_in(own, 3), amount)
    donor, sink = mixed[0:amount // 2 * 2:2], mixed[1:amount // 2 * 2:2]
    margin = jnp.minimum(sizes[donor] - 1, reach - sizes[sink]) // 2
    margin = jnp.where((donor == sequence[0]) | (sink == sequence[0]) | (sizes[sink] == 0), 0, jnp.maximum(margin, 0))
    shifted = jax.random.randint(jax.random.fold_in(own, 4), (amount // 2,), 0, 1 << 20) % (margin + 1)
    sizes = sizes.at[donor].add(-shifted).at[sink].add(shifted)
    items = jnp.searchsorted(jnp.cumsum(sizes), jnp.arange(rows * top), side="right").astype(jnp.int32)
    grid = items.reshape(top, rows).T
    grid = grid[jax.random.permutation(jax.random.fold_in(own, 1), rows)]
    rotation = jax.random.randint(jax.random.fold_in(own, 2), (rows, 1), 0, top)
    return jnp.take_along_axis(grid, (jnp.arange(top)[None, :] + rotation) % top, axis=1)


def shares(count, total, reach, slope, full):
    weights = [(1 << 20) // math.isqrt(rank ** slope) + 1 for rank in range(1, count + 1)]
    largest = reach if full else min(reach, max(-(-total // count), total * weights[0] // sum(weights)))
    least = 1 if total - largest >= count - 1 else 0
    given, spare = [largest] + [least] * (count - 1), total - largest - least * (count - 1)
    while spare > 0:
        candidates = [i for i in range(1, count) if given[i] < largest] or [i for i in range(1, count) if given[i] < reach]
        mass, remaining = sum([weights[i] for i in candidates]), spare
        for i in candidates:
            addition = min(reach - given[i], max(1, remaining * weights[i] // mass), spare)
            given[i] = given[i] + addition
            spare = spare - addition
    return np.array(given)


def normal_values(rng, extent, scale, bound, cuts=(), kind=jnp.bfloat16):
    entries = jax.random.normal(rng, extent, jnp.float32) * scale
    if len(cuts) > 0:
        entries = levels(rng, extent, cuts, -0.22, 0.18) * entries
    return jnp.clip(entries, min=-bound, max=bound).astype(kind)


def setup_inputs(seed: int = 0) -> dict:
    splits = jax.random.split(jax.random.key(seed), 11)
    patches = normal_values(splits[0], (N_CLIENT * IMG * TOK, PATCH), 1.0, 6.0, ((0, 32),))
    labels = place_ends(jax.random.randint(splits[1], (N_CLIENT * IMG,), 0, CLASSES), jax.random.fold_in(splits[1], 1), 0, CLASSES - 1).astype(jnp.int32)
    assign_keys = jax.random.split(jax.random.fold_in(splits[2], 1), N_CLIENT // N_CLIENT)
    assign_turns = jax.random.permutation(jax.random.fold_in(splits[2], 3), N_CLIENT // N_CLIENT)
    assign = jax.vmap(lambda own, number: assign_block(jax.random.fold_in(splits[2], 2), own, number, N_CLIENT, SHARDS, 1, CAPACITY, 2))(assign_keys, assign_turns).reshape((N_CLIENT, 1))
    patch_embed = normal_values(splits[3], (PATCH, D), PATCH ** -0.5, 0.4375)
    positions = normal_values(splits[4], (TOK, D), 0.5, 3.0)
    client_in = draw_client_in(jax.random.fold_in(splits[10], 71), 0)
    client_down = normal_values(splits[6], (FF, D), FF ** -0.5, 0.15625)
    server_in = draw_server_in(jax.random.fold_in(splits[10], 71), 0)
    server_down = normal_values(splits[8], (SERVER_LAYERS, SHARDS * FF, D), FF ** -0.5, 0.15625, ((1, 32),))
    classifier = draw_classifier(jax.random.fold_in(splits[10], 71), 0)
    return dict(patches=patches, labels=labels, assign=assign, patch_embed=patch_embed, positions=positions, client_in=client_in, client_down=client_down, server_in=server_in, server_down=server_down, classifier=classifier)


EPSILON = 1e-06

def layer_norm(inputs):
    centre = inputs - lax.optimization_barrier(jnp.mean(inputs, axis=-1, keepdims=True))
    spread = lax.optimization_barrier(jnp.mean(centre * centre, axis=-1, keepdims=True))
    return centre * lax.rsqrt(spread + EPSILON)

def encoder_block(stream, weight_in, weight_down):
    images, tokens, model_width = stream.shape
    head_dim = model_width // HEADS
    normed = layer_norm(stream).astype(jnp.bfloat16).reshape(images * tokens, model_width)
    projected = jnp.dot(normed, weight_in[:, :3 * model_width], preferred_element_type=jnp.float32)
    projected = projected.reshape(images, tokens, 3, HEADS, head_dim)
    queries = projected[:, :, 0]
    key_rows = projected[:, :, 1]
    values = projected[:, :, 2]
    scores = jnp.einsum('bqhe,bkhe->bhqk', queries, key_rows, precision=lax.Precision.HIGHEST) / math.sqrt(head_dim)
    weights_attn = jax.nn.softmax(scores, axis=-1)
    attended = jnp.einsum('bhqk,bkhe->bqhe', weights_attn, values, precision=lax.Precision.HIGHEST)
    attended = attended.reshape(images * tokens, model_width).astype(jnp.bfloat16)
    stream = stream + jnp.dot(attended, weight_in[:, 3 * model_width:4 * model_width], preferred_element_type=jnp.float32).reshape(images, tokens, model_width)
    normed = layer_norm(stream).astype(jnp.bfloat16).reshape(images * tokens, model_width)
    hidden = jax.nn.gelu(jnp.dot(normed, weight_in[:, 4 * model_width:], preferred_element_type=jnp.float32)).astype(jnp.bfloat16)
    return stream + jnp.dot(hidden, weight_down, preferred_element_type=jnp.float32).reshape(images, tokens, model_width)

def client_forward(patch_rows, patch_embed, positions, client_in, client_down):
    stream = jnp.dot(patch_rows, patch_embed, preferred_element_type=jnp.float32).reshape(-1, TOK, D)
    stream = stream + positions.astype(jnp.float32)
    stream = encoder_block(stream, client_in, client_down)
    return stream.reshape(-1, D).astype(jnp.bfloat16)

def server_loss(cut_rows, slot_hot, weights_in, weights_down, class_shard):
    stream = cut_rows.astype(jnp.float32).reshape(-1, TOK, D)
    for layer in range(len(weights_in)):
        stream = encoder_block(stream, weights_in[layer], weights_down[layer])
    pooled = layer_norm(lax.optimization_barrier(jnp.mean(stream, axis=1))).astype(jnp.bfloat16)
    logits = jnp.dot(pooled, class_shard, preferred_element_type=jnp.float32)
    per_loss = (jax.nn.logsumexp(logits, axis=-1) - lax.optimization_barrier(jnp.sum(slot_hot * logits, axis=-1))) * lax.optimization_barrier(jnp.sum(slot_hot, axis=-1))
    return (jnp.sum(per_loss), per_loss)

def arrival_rank(routes):
    places = jnp.arange(routes.shape[0], dtype=jnp.int32)
    earlier = (routes[:, None] == routes[None, :]) & (places[:, None] < places[None, :])
    return lax.optimization_barrier(jnp.sum(earlier.astype(jnp.int32), axis=0))

def select_matrix(routes, arrival, shard, capacity):
    slots_here = jnp.arange(capacity, dtype=jnp.int32)[:, None]
    return ((routes[None, :] == shard) & (arrival[None, :] == slots_here)).astype(jnp.bfloat16)

def slot_labels(labels, selector, rank_in_group, per_image, members):
    label_table = labels.reshape(members, IMG)
    label_part = lax.dynamic_slice_in_dim(label_table, (rank_in_group * per_image).astype(jnp.int32), per_image, 1)
    onehot = (label_part[:, :, None] == jnp.arange(CLASSES, dtype=jnp.int32)[None, None, :]).astype(jnp.float32)
    onehot = onehot.reshape(members, per_image * CLASSES)
    chosen = jnp.dot(selector.astype(jnp.float32), onehot, precision=lax.Precision.HIGHEST)
    return chosen.reshape(-1, CLASSES)

def reference(patches, labels, assign, patch_embed, positions, client_in, client_down, server_in, server_down, classifier):
    members = N_CLIENT
    group_size = members // SHARDS
    per_image = IMG // group_size
    piece_rows = IMG * TOK // group_size
    capacity = SLOTS * group_size
    width_all = 4 * D + FF
    routes = assign[:, 0]
    arrival = arrival_rank(routes)
    patch_sets = patches.reshape(members, IMG * TOK, PATCH)

    def client_cut(patch_rows):
        return client_forward(patch_rows, patch_embed, positions, client_in, client_down)
    cuts = lax.map(client_cut, patch_sets)
    cut_pieces = cuts.reshape(members, group_size, piece_rows * D)
    shard_in = server_in.reshape(SERVER_LAYERS, SHARDS, D, width_all)
    shard_down = server_down.reshape(SERVER_LAYERS, SHARDS, FF, D)

    def device_step(carry, device):
        acc_in, acc_down, acc_class = carry
        shard = device // group_size
        rank_in_group = device % group_size
        selector = select_matrix(routes, arrival, shard, capacity)
        own_piece = lax.dynamic_index_in_dim(cut_pieces, rank_in_group, 1, keepdims=False)
        compact = jnp.dot(selector, own_piece, preferred_element_type=jnp.float32).astype(jnp.bfloat16)
        compact = compact.reshape(capacity * piece_rows, D)
        slot_hot = slot_labels(labels, selector, rank_in_group, per_image, members)
        layer_in = lax.dynamic_index_in_dim(shard_in, shard, 1, keepdims=False)
        layer_down = lax.dynamic_index_in_dim(shard_down, shard, 1, keepdims=False)
        class_shard = lax.dynamic_index_in_dim(classifier, shard, 0, keepdims=False)

        def loss_of(cut_rows, weights_in, weights_down, class_weights):
            return server_loss(cut_rows, slot_hot, weights_in, weights_down, class_weights)
        list_in = tuple((layer_in[layer] for layer in range(SERVER_LAYERS)))
        list_down = tuple((layer_down[layer] for layer in range(SERVER_LAYERS)))
        total_loss, server_back, per_loss = jax.vjp(loss_of, compact, list_in, list_down, class_shard, has_aux=True)
        grad_cut, grad_in, grad_down, grad_class = server_back(jnp.ones((), jnp.float32))
        acc_in = acc_in.at[:, shard].add(jnp.stack(grad_in).astype(jnp.float32))
        acc_down = acc_down.at[:, shard].add(jnp.stack(grad_down).astype(jnp.float32))
        acc_class = acc_class.at[shard].add(grad_class.astype(jnp.float32))
        return ((acc_in, acc_down, acc_class), (grad_cut, per_loss))
    start = (jnp.zeros((SERVER_LAYERS, SHARDS, D, width_all), jnp.float32), jnp.zeros((SERVER_LAYERS, SHARDS, FF, D), jnp.float32), jnp.zeros((SHARDS, D, CLASSES), jnp.float32))
    sums, outputs = lax.scan(device_step, start, jnp.arange(members, dtype=jnp.int32))
    acc_in, acc_down, acc_class = sums
    cut_grads, loss_rows = outputs
    cut_grads = cut_grads.reshape(SHARDS, group_size, capacity, piece_rows * D)

    def client_step(carry, client):
        shard = routes[client]
        slot = arrival[client]
        by_shard = lax.dynamic_index_in_dim(cut_grads, shard, 0, keepdims=False)
        own_grads = lax.dynamic_index_in_dim(by_shard, slot, 1, keepdims=False).reshape(IMG * TOK, D)
        patch_rows = lax.dynamic_index_in_dim(patch_sets, client, 0, keepdims=False)

        def client_of(embed_weights, position_weights, in_weights, down_weights):
            return client_forward(patch_rows, embed_weights, position_weights, in_weights, down_weights)
        cut_again, client_back = jax.vjp(client_of, patch_embed, positions, client_in, client_down)
        grads = client_back(own_grads)
        return (tuple((total + part_grad.astype(jnp.float32) for total, part_grad in zip(carry, grads))), None)
    client_start = (jnp.zeros((PATCH, D), jnp.float32), jnp.zeros((TOK, D), jnp.float32), jnp.zeros((D, width_all), jnp.float32), jnp.zeros((FF, D), jnp.float32))
    client_sums, unused = lax.scan(client_step, client_start, jnp.arange(members, dtype=jnp.int32))
    return (loss_rows, client_sums[0], client_sums[1], client_sums[2], client_sums[3], acc_in.reshape(SERVER_LAYERS, SHARDS * D, width_all), acc_down.reshape(SERVER_LAYERS, SHARDS * FF, D), acc_class.reshape(SHARDS * D, CLASSES))
```

```python
import functools
import math

import jax
import jax.numpy as jnp
from jax import lax
from jax.experimental import pallas as pl
from jax.experimental.pallas import tpu as pltpu
from jax.sharding import PartitionSpec as P

HEADS = 6
TOK = 16
IMG = 8
SHARDS = 16
SLOTS = 2
PLANE = 4
EPSILON = 1e-06
LANES = 128
PAD = 16
BF = jnp.bfloat16
F32 = jnp.float32
HIGH = lax.Precision.HIGHEST
GELU_C = math.sqrt(2.0 / math.pi)
VMEM_LIMIT = 60 * 1024 * 1024
MESH = pl.DeviceIdType.MESH


def mm(a, b, precision=None):
    return lax.dot_general(
        a, b, (((1,), (0,)), ((), ())), precision=precision, preferred_element_type=F32
    )


def mm_nt(a, b, precision=None):
    return lax.dot_general(
        a, b, (((1,), (1,)), ((), ())), precision=precision, preferred_element_type=F32
    )


def mm_tn(a, b):
    return lax.dot_general(a, b, (((0,), (0,)), ((), ())), preferred_element_type=F32)


def norm(v):
    centre = v - jnp.mean(v, axis=-1, keepdims=True)
    scale = lax.rsqrt(jnp.mean(centre * centre, axis=-1, keepdims=True) + EPSILON)
    return centre * scale, scale


def norm_back(normed, scale, grad):
    return scale * (
        grad
        - jnp.mean(grad, axis=-1, keepdims=True)
        - normed * jnp.mean(grad * normed, axis=-1, keepdims=True)
    )


def gelu(v):
    t = jnp.tanh(GELU_C * (v + 0.044715 * (v * v * v)))
    return 0.5 * v * (1.0 + t)


def gelu_both(v):
    sq = v * v
    t = jnp.tanh(GELU_C * (v + 0.044715 * (sq * v)))
    value = 0.5 * v * (1.0 + t)
    slope = 0.5 * (1.0 + t) + 0.5 * v * (1.0 - t * t) * (GELU_C * (1.0 + 0.134145 * sq))
    return value, slope


def image_mask():
    row = lax.broadcasted_iota(jnp.int32, (LANES, LANES), 0)
    col = lax.broadcasted_iota(jnp.int32, (LANES, LANES), 1)
    return row // TOK == col // TOK


def lane_masks(head_dim):
    lane = lax.broadcasted_iota(jnp.int32, (LANES, LANES), 1)
    return [lane // head_dim == h for h in range(LANES // head_dim)]


def attend(qkv_ref, probs_ref, att_ref, width):
    rows = qkv_ref.shape[0]
    head_dim = width // HEADS
    per = LANES // head_dim
    inside = image_mask()
    keeps = lane_masks(head_dim)
    for group in range(rows // LANES):
        r = slice(group * LANES, (group + 1) * LANES)
        for pair in range(width // LANES):
            lo = pair * LANES
            q = qkv_ref[r, lo : lo + LANES]
            k = qkv_ref[r, width + lo : width + lo + LANES]
            v = qkv_ref[r, 2 * width + lo : 2 * width + lo + LANES]
            out = jnp.zeros((LANES, LANES), F32)
            for h in range(per):
                s = mm_nt(jnp.where(keeps[h], q, 0.0), k, HIGH) * (1.0 / math.sqrt(head_dim))
                s = jnp.where(inside, s, -1e30)
                e = jnp.exp(s - jnp.max(s, axis=-1, keepdims=True))
                p = (e / jnp.sum(e, axis=-1, keepdims=True)).astype(BF)
                probs_ref[group * HEADS + pair * per + h] = p
                out = out + mm(p, jnp.where(keeps[h], v, 0.0).astype(BF))
            att_ref[r, lo : lo + LANES] = out.astype(BF)


def attend_back(grad, qkv_ref, probs_ref, dqkv_ref, width):
    rows = qkv_ref.shape[0]
    head_dim = width // HEADS
    per = LANES // head_dim
    keeps = lane_masks(head_dim)
    for group in range(rows // LANES):
        r = slice(group * LANES, (group + 1) * LANES)
        for pair in range(width // LANES):
            lo = pair * LANES
            q = qkv_ref[r, lo : lo + LANES]
            k = qkv_ref[r, width + lo : width + lo + LANES]
            v = qkv_ref[r, 2 * width + lo : 2 * width + lo + LANES].astype(BF)
            go = grad[r, lo : lo + LANES]
            dq = jnp.zeros((LANES, LANES), F32)
            dk = jnp.zeros((LANES, LANES), F32)
            dv = jnp.zeros((LANES, LANES), F32)
            for h in range(per):
                p = probs_ref[group * HEADS + pair * per + h]
                goh = jnp.where(keeps[h], go, 0.0).astype(BF)
                dp = mm_nt(goh, v)
                dv = dv + mm_tn(p, goh)
                pf = p.astype(F32)
                ds = pf * (dp - jnp.sum(pf * dp, axis=-1, keepdims=True))
                ds = (ds * (1.0 / math.sqrt(head_dim))).astype(BF)
                dq = dq + mm(ds, jnp.where(keeps[h], k, 0.0).astype(BF))
                dk = dk + mm_tn(ds, jnp.where(keeps[h], q, 0.0).astype(BF))
            dqkv_ref[r, lo : lo + LANES] = dq.astype(BF)
            dqkv_ref[r, width + lo : width + lo + LANES] = dk.astype(BF)
            dqkv_ref[r, 2 * width + lo : 2 * width + lo + LANES] = dv.astype(BF)


def block_forward(x, w_ref, d_ref, qkv_ref, probs_ref, att_ref, mid_ref, pre_ref):
    width = x.shape[1]
    u = norm(x)[0].astype(BF)
    qkv_ref[...] = mm(u, w_ref[:, : 3 * width])
    attend(qkv_ref, probs_ref, att_ref, width)
    y = x + mm(att_ref[...], w_ref[:, 3 * width : 4 * width])
    mid_ref[...] = y
    u = norm(y)[0].astype(BF)
    pre_ref[...] = mm(u, w_ref[:, 4 * width :])
    h = gelu(pre_ref[...]).astype(BF)
    return y + mm(h, d_ref[...])


def block_backward(
    g, x, w_ref, d_ref, qkv_ref, probs_ref, att_ref, mid_ref, pre_ref, dqkv_ref, put_in, put_down
):
    width = x.shape[1]
    gb = g.astype(BF)
    h, slope = gelu_both(pre_ref[...])
    put_down(h.astype(BF), gb)
    dpre = (mm_nt(gb, d_ref[...]) * slope).astype(BF)
    y = mid_ref[...]
    u, scale = norm(y)
    put_in(4 * width, u.astype(BF), dpre)
    dy = g + norm_back(u, scale, mm_nt(dpre, w_ref[:, 4 * width :]))
    gb = dy.astype(BF)
    put_in(3 * width, att_ref[...], gb)
    attend_back(
        mm_nt(gb, w_ref[:, 3 * width : 4 * width]), qkv_ref, probs_ref, dqkv_ref, width
    )
    u, scale = norm(x)
    dqkv = dqkv_ref[...]
    put_in(0, u.astype(BF), dqkv)
    return dy + norm_back(u, scale, mm_nt(dqkv, w_ref[:, : 3 * width]))


def bits_of(n):
    return n.bit_length() - 1


def part_orders(n):
    rest = list(range(1, bits_of(n)))
    far = rest[-2:]
    near = rest[:-2]
    low = near[: len(near) // 2]
    high = near[len(near) // 2 :]
    return [[0] + low + high + far, [0] + high + low + far, [0] + far + low + high]


def place_of(device, order):
    index = 0
    for bit in order:
        index = index * 2 + (device >> bit & 1)
    return index


def split_rows(r_in):
    return r_in - PAD if r_in >= 4 * PAD else r_in


def gather_kernel(
    n, group, capacity,
    assign_ref, patch_ref,
    slots_ref, table_ref,
    column, pack, got, near_send, near_recv, far_send, far_recv, flat_send, flat_recv,
):
    me = lax.axis_index("client")
    rank = me % group
    shard = me // group
    line = shard // PLANE
    spot = shard % PLANE
    barrier = pltpu.get_barrier_semaphore()

    def near_peer(i):
        return shard * group + lax.rem(rank + i, group)

    def far_peer(i):
        return (lax.rem(line + i, PLANE) * PLANE + spot) * group + rank

    def flat_peer(i):
        return (line * PLANE + lax.rem(spot + i, PLANE)) * group + rank

    peers = [near_peer(i) for i in range(1, group)]
    peers += [far_peer(i) for i in range(1, PLANE)]
    peers += [flat_peer(i) for i in range(1, PLANE)]
    for peer in peers:
        pl.semaphore_signal(barrier, inc=1, device_id=(peer,), device_id_type=MESH)
    pl.semaphore_wait(barrier, len(peers))

    def near(i):
        to = lax.rem(rank + i, group)
        return pltpu.make_async_remote_copy(
            src_ref=patch_ref.at[to], dst_ref=column.at[line, rank], send_sem=near_send.at[i],
            recv_sem=near_recv.at[i], device_id=(near_peer(i),), device_id_type=MESH,
        )

    def far(i, j):
        if j == 0:
            source, member = patch_ref.at[rank], rank
        else:
            member = lax.rem(rank + group - j, group)
            source = column.at[line, member]
        return pltpu.make_async_remote_copy(
            src_ref=source, dst_ref=column.at[line, member], send_sem=far_send.at[i, j],
            recv_sem=far_recv.at[i, j], device_id=(far_peer(i),), device_id_type=MESH,
        )

    def flat(i):
        return pltpu.make_async_remote_copy(
            src_ref=pack.at[i], dst_ref=got.at[spot], send_sem=flat_send.at[i],
            recv_sem=flat_recv.at[i], device_id=(flat_peer(i),), device_id_type=MESH,
        )

    for i in range(1, group):
        near(i).start()
    for i in range(1, PLANE):
        far(i, 0).start()
    for j in range(1, group):
        near(j).wait_recv()
        for i in range(1, PLANE):
            far(i, j).start()
    column[line, rank] = patch_ref[rank]

    targets = [line * PLANE + lax.rem(spot + i, PLANE) for i in range(PLANE)]

    def scan(c, carry):
        there = assign_ref[c]
        out = []
        for i in range(PLANE):
            count, slots = carry[i]
            hit = there == targets[i]
            slots = tuple(
                jnp.where(hit & (count == k), c, slots[k]) for k in range(capacity)
            )
            out.append((count + jnp.where(hit, 1, 0), slots))
        return tuple(out)

    zero = jnp.int32(0)
    table = lax.fori_loop(
        0, n, scan, tuple((zero, tuple(zero for _ in range(capacity))) for _ in range(PLANE))
    )
    for i in range(1, PLANE):
        for j in range(group):
            far(i, j).wait_recv()

    def pick(c):
        home = c // group
        return column[home // PLANE, c % group]

    for i in range(1, PLANE):
        for k in range(capacity):
            pack[i, k] = pick(table[i][1][k])
    for i in range(1, PLANE):
        flat(i).start()
    count, slots = table[0]
    for k in range(capacity):
        got[spot, k] = pick(slots[k])
        table_ref[k] = slots[k]
    table_ref[capacity] = count
    for i in range(1, PLANE):
        flat(i).wait_recv()
    piece = patch_ref.shape[1]
    for k in range(capacity):
        home = slots[k] // group
        slots_ref[k * piece : (k + 1) * piece, :] = got[home % PLANE, k]
    for i in range(1, group):
        near(i).wait_send()
    for i in range(1, PLANE):
        for j in range(group):
            far(i, j).wait_send()
        flat(i).wait_send()


def step_kernel(
    n, group, layers, per_image, capacity, classes, *refs,
):
    table_ref, label_ref, patch_ref, embed_ref, pos_ref, class_ref, cin_ref, cdown_ref = refs[:8]
    refs = refs[8:]
    in_pieces, refs = refs[:group], refs[group:]
    down_pieces, refs = refs[:group], refs[group:]
    loss_ref, gclass_ref, pack_a, pack_b, pack_c = refs[:5]
    refs = refs[5:]
    gin_out, refs = refs[:group], refs[group:]
    gdown_out, refs = refs[:group], refs[group:]
    (
        wbuf, dbuf, gin, gdown, xs, qkv, probs, att, mid, pre, dqkv, gcur, cls,
        w_sem, g_sem, c_sem,
    ) = refs
    me = lax.axis_index("client")
    rank = me % group
    shard = me // group
    rows_in = in_pieces[0].shape[1]
    rows_down = down_pieces[0].shape[1]
    rows, width = gcur.shape
    ff = dbuf.shape[1]

    def client_copies():
        return [
            pltpu.make_async_copy(cin_ref, wbuf.at[0], c_sem.at[0]),
            pltpu.make_async_copy(cdown_ref, dbuf.at[0], c_sem.at[1]),
        ]

    def class_copy():
        return pltpu.make_async_copy(class_ref.at[shard], cls, c_sem.at[2])

    def weight_copies(layer):
        made = []
        for i in range(group):
            who = rank ^ i
            made.append(pltpu.make_async_copy(
                in_pieces[i].at[layer],
                wbuf.at[layer + 1, pl.ds(pl.multiple_of(who * rows_in, rows_in), rows_in)],
                w_sem.at[layer, 2 * i],
            ))
            made.append(pltpu.make_async_copy(
                down_pieces[i].at[layer],
                dbuf.at[layer + 1, pl.ds(pl.multiple_of(who * rows_down, rows_down), rows_down)],
                w_sem.at[layer, 2 * i + 1],
            ))
        return made

    def grad_copies(layer):
        made = []
        for i in range(group):
            who = rank ^ i
            made.append(pltpu.make_async_copy(
                gin.at[layer, pl.ds(pl.multiple_of(who * rows_in, rows_in), rows_in)],
                gin_out[i].at[layer],
                g_sem.at[layer, 2 * i],
            ))
            made.append(pltpu.make_async_copy(
                gdown.at[layer, pl.ds(pl.multiple_of(who * rows_down, rows_down), rows_down)],
                gdown_out[i].at[layer],
                g_sem.at[layer, 2 * i + 1],
            ))
        return made

    for c in client_copies():
        c.start()
    class_copy().start()
    for layer in range(layers):
        for c in weight_copies(layer):
            c.start()

    images = capacity * per_image
    row = lax.broadcasted_iota(jnp.int32, (images, classes), 0)
    lane = lax.broadcasted_iota(jnp.int32, (images, classes), 1)
    want = jnp.full((images, classes), -1, jnp.int32)
    filled = table_ref[capacity]
    for k in range(capacity):
        base = table_ref[k] * (group * per_image) + rank * per_image
        for j in range(per_image):
            lab = jnp.where(k < filled, label_ref[base + j], -1)
            want = jnp.where(row == k * per_image + j, lab, want)
    hot = (lane == want).astype(F32)
    full = (want[:, :1] >= 0).astype(F32)

    x = mm(patch_ref[...], embed_ref[...])
    pos = pos_ref[...].astype(F32)
    xs[0] = x + jnp.concatenate([pos] * (rows // TOK), axis=0)
    for c in client_copies():
        c.wait()

    def forward(layer, carry):
        @pl.when(layer > 0)
        def _():
            for c in weight_copies(layer - 1):
                c.wait()

        out = block_forward(
            xs[layer], wbuf.at[layer], dbuf.at[layer], qkv.at[layer], probs.at[layer],
            att.at[layer], mid.at[layer], pre.at[layer],
        )
        xs[layer + 1] = jnp.where(layer == 0, out.astype(BF).astype(F32), out)
        return carry

    lax.fori_loop(0, layers + 1, forward, 0)

    pool = (
        lax.broadcasted_iota(jnp.int32, (images, rows), 1) // TOK
        == lax.broadcasted_iota(jnp.int32, (images, rows), 0)
    ).astype(F32) * (1.0 / TOK)
    unpool = (
        lax.broadcasted_iota(jnp.int32, (rows, images), 0) // TOK
        == lax.broadcasted_iota(jnp.int32, (rows, images), 1)
    ).astype(F32) * (1.0 / TOK)
    class_copy().wait()
    u, scale = norm(mm(pool, xs[layers + 1], HIGH))
    pooled = u.astype(BF)
    logits = mm(pooled, cls[...])
    top = jnp.max(logits, axis=-1, keepdims=True)
    e = jnp.exp(logits - top)
    total = jnp.sum(e, axis=-1, keepdims=True)
    loss = (
        jnp.log(total) + top - jnp.sum(jnp.where(lane == want, logits, 0.0), axis=-1, keepdims=True)
    ) * full
    eye = (
        lax.broadcasted_iota(jnp.int32, (images, images), 0)
        == lax.broadcasted_iota(jnp.int32, (images, images), 1)
    )
    loss_ref[...] = jnp.sum(jnp.where(eye, loss, 0.0), axis=0, keepdims=True)
    dlog = ((e / total - hot) * full).astype(BF)
    gclass_ref[...] = mm_tn(pooled, dlog).astype(BF)
    dpool = norm_back(u, scale, mm_nt(dlog, cls[...]))
    gcur[...] = mm(unpool, dpool, HIGH)

    def backward(i, carry):
        layer = layers - 1 - i

        def put_in(start, lhs, rhs):
            gin[layer, :, start : start + rhs.shape[1]] = mm_tn(lhs, rhs).astype(BF)

        def put_down(h, gb):
            gdown[layer] = mm_tn(h, gb).astype(BF)

        deep = layer + 1
        gcur[...] = block_backward(
            gcur[...], xs[deep], wbuf.at[deep], dbuf.at[deep], qkv.at[deep],
            probs.at[deep], att.at[deep], mid.at[deep], pre.at[deep], dqkv,
            put_in, put_down,
        )
        for c in grad_copies(layer):
            c.start()
        return carry

    lax.fori_loop(0, layers, backward, 0)

    orders = part_orders(n)
    per_dev = wbuf.shape[2] // n
    head = split_rows(per_dev)
    cols = width // n
    src = lax.broadcasted_iota(jnp.int32, (width, n * PAD), 0)
    dst = lax.broadcasted_iota(jnp.int32, (width, n * PAD), 1)
    spread_to = ((dst // PAD == src // cols) & (dst % PAD == src % cols)).astype(F32).astype(BF)
    tok = (
        lax.broadcasted_iota(jnp.int32, (rows, LANES), 0) % TOK
        == lax.broadcasted_iota(jnp.int32, (rows, LANES), 1)
    ).astype(F32).astype(BF)

    def put_in(start, lhs, rhs):
        for c in range(0, rhs.shape[1], width):
            part = mm_tn(rhs[:, c : c + width], lhs).astype(BF)
            first = (start + c) // per_dev
            for j in range(width // per_dev):
                lo = j * per_dev
                pack_a[place_of(first + j, orders[0])] = part[lo : lo + head]
                if head < per_dev:
                    pack_b[place_of(first + j, orders[1]), : per_dev - head] = (
                        part[lo + head : lo + per_dev]
                    )

    def put_down(h, gb):
        spread = mm(gb, spread_to).astype(BF)
        last = ff // width - 1
        for q in range(ff // width):
            part = mm_tn(spread, h[:, q * width : (q + 1) * width]).astype(BF)
            lo = per_dev - head + q * PAD
            for j in range(n):
                value = part[j * PAD : (j + 1) * PAD]
                if q == last:
                    pack_c[place_of(j, orders[2]), :PAD] = value
                else:
                    pack_b[place_of(j, orders[1]), lo : lo + PAD] = value

    dx = block_backward(
        gcur[...].astype(BF).astype(F32), xs[0], wbuf.at[0], dbuf.at[0], qkv.at[0],
        probs.at[0], att.at[0], mid.at[0], pre.at[0], dqkv, put_in, put_down,
    )
    spread = mm(dx.astype(BF), spread_to).astype(BF)
    patch = patch_ref.shape[1]
    embed_part = mm_tn(spread, patch_ref[...]).astype(BF)
    pos_part = mm_tn(spread, tok).astype(BF)
    for j in range(n):
        at = place_of(j, orders[2])
        pack_c[at, PAD : 2 * PAD, :patch] = embed_part[j * PAD : (j + 1) * PAD]
        pack_c[at, PAD : 2 * PAD, patch : width - LANES] = jnp.zeros(
            (PAD, width - LANES - patch), BF
        )
        pack_c[at, PAD : 2 * PAD, width - LANES :] = pos_part[j * PAD : (j + 1) * PAD]

    for layer in range(layers):
        for c in grad_copies(layer):
            c.wait()


def reduce_kernel(n, *refs):
    steps = bits_of(n)
    orders = part_orders(n)
    parts = len(orders)
    packs, refs = refs[:parts], refs[parts:]
    outs, refs = refs[:parts], refs[parts:]
    got = [refs[q * steps : (q + 1) * steps] for q in range(parts)]
    refs = refs[parts * steps :]
    held = [refs[q * (steps - 1) : (q + 1) * (steps - 1)] for q in range(parts)]
    send_sem, recv_sem = refs[parts * (steps - 1) :]
    me = lax.axis_index("client")
    barrier = pltpu.get_barrier_semaphore()

    def peer(bit):
        return me + (1 << bit) - 2 * (1 << bit) * (me // (1 << bit) % 2)

    for bit in range(steps):
        pl.semaphore_signal(barrier, inc=1, device_id=(peer(bit),), device_id_type=MESH)
    pl.semaphore_wait(barrier, steps)

    def source(q, t):
        return packs[q] if t == 0 else held[q][t - 1]

    def mine(q, t):
        return me // (1 << orders[q][t]) % 2

    def copy(q, t):
        half = n >> (t + 1)
        return pltpu.make_async_remote_copy(
            src_ref=source(q, t).at[pl.ds((1 - mine(q, t)) * half, half)], dst_ref=got[q][t],
            send_sem=send_sem.at[q, t], recv_sem=recv_sem.at[q, t],
            device_id=(peer(orders[q][t]),), device_id_type=MESH,
        )

    for q in range(parts):
        copy(q, 0).start()
    for t in range(steps):
        half = n >> (t + 1)
        for q in range(parts):
            copy(q, t).wait_recv()
            first = mine(q, t) * half
            if t == steps - 1:
                outs[q][...] = source(q, t)[first].astype(F32) + got[q][t][0].astype(F32)
            else:
                def add(e, carry, q=q, t=t, first=first):
                    held[q][t][e] = (
                        source(q, t)[first + e].astype(F32) + got[q][t][e].astype(F32)
                    ).astype(BF)
                    return carry

                lax.fori_loop(0, half, add, 0)
                copy(q, t + 1).start()
    for t in range(steps):
        for q in range(parts):
            copy(q, t).wait_send()


def vmem():
    return pl.BlockSpec(memory_space=pltpu.VMEM)


def smem():
    return pl.BlockSpec(memory_space=pltpu.SMEM)


def hbm():
    return pl.BlockSpec(memory_space=pl.ANY)


def shape(dims, kind):
    return jax.ShapeDtypeStruct(dims, kind)


def flip(block, bit):
    n = lax.axis_size("client")
    return lax.ppermute(block, "client", [(i, i ^ (1 << bit)) for i in range(n)])


def per_device(
    patches, labels, assign, patch_embed, positions, client_in, client_down,
    server_in, server_down, classifier,
):
    n = lax.axis_size("client")
    group = n // SHARDS
    bits = group.bit_length() - 1
    me = lax.axis_index("client")
    rank = me % group
    rows = patches.shape[0]
    patch = patches.shape[1]
    width = client_in.shape[0]
    cols = client_in.shape[1]
    ff = client_down.shape[0]
    layers = server_in.shape[0]
    rows_in = server_in.shape[1]
    rows_down = server_down.shape[1]
    classes = classifier.shape[2]
    piece = rows // group
    per_image = IMG // group
    capacity = SLOTS * group
    s_rows = capacity * piece
    routes = assign.reshape(n)
    params = pltpu.CompilerParams(vmem_limit_bytes=VMEM_LIMIT)

    in_pieces = [server_in]
    down_pieces = [server_down]
    for bit in range(bits):
        in_pieces = in_pieces + [flip(p, bit) for p in in_pieces]
        down_pieces = down_pieces + [flip(p, bit) for p in down_pieces]

    slots, table = pl.pallas_call(
        functools.partial(gather_kernel, n, group, capacity),
        out_shape=[shape((s_rows, patch), BF), shape((capacity + 1,), jnp.int32)],
        in_specs=[smem(), vmem()],
        out_specs=[vmem(), smem()],
        scratch_shapes=[
            pltpu.VMEM((PLANE, group, piece, patch), BF),
            pltpu.VMEM((PLANE, capacity, piece, patch), BF),
            pltpu.VMEM((PLANE, capacity, piece, patch), BF),
            pltpu.SemaphoreType.DMA((group,)),
            pltpu.SemaphoreType.DMA((group,)),
            pltpu.SemaphoreType.DMA((PLANE, group)),
            pltpu.SemaphoreType.DMA((PLANE, group)),
            pltpu.SemaphoreType.DMA((PLANE,)),
            pltpu.SemaphoreType.DMA((PLANE,)),
        ],
        compiler_params=pltpu.CompilerParams(
            collective_id=1, has_side_effects=True, vmem_limit_bytes=VMEM_LIMIT
        ),
    )(routes, patches.reshape(group, piece, patch))

    def kept(r):
        return [
            shape((r, 3 * width), F32),
            shape((r // LANES * HEADS, LANES, LANES), BF),
            shape((r, width), BF),
            shape((r, width), F32),
            shape((r, ff), F32),
        ]

    r_in = cols // n
    head = split_rows(r_in)
    tall = [head, r_in - head + (ff // width - 1) * PAD, 2 * PAD]
    part_in = shape((layers, rows_in, cols), BF)
    part_down = shape((layers, rows_down, width), BF)
    res = pl.pallas_call(
        functools.partial(step_kernel, n, group, layers, per_image, capacity, classes),
        out_shape=[
            shape((1, capacity * per_image), F32),
            shape((width, classes), BF),
        ]
        + [shape((n, r, width), BF) for r in tall]
        + [part_in] * group
        + [part_down] * group,
        in_specs=[smem(), smem()] + [vmem()] * 3 + [hbm()] * (3 + 2 * group),
        out_specs=[vmem()] * 5 + [hbm()] * (2 * group),
        scratch_shapes=[
            pltpu.VMEM((layers + 1, width, cols), BF),
            pltpu.VMEM((layers + 1, ff, width), BF),
            pltpu.VMEM((layers, width, cols), BF),
            pltpu.VMEM((layers, ff, width), BF),
            pltpu.VMEM((layers + 2, s_rows, width), F32),
        ]
        + [pltpu.VMEM((layers + 1,) + s.shape, s.dtype) for s in kept(s_rows)]
        + [
            pltpu.VMEM((s_rows, 3 * width), BF),
            pltpu.VMEM((s_rows, width), F32),
            pltpu.VMEM((width, classes), BF),
            pltpu.SemaphoreType.DMA((layers, 2 * group)),
            pltpu.SemaphoreType.DMA((layers, 2 * group)),
            pltpu.SemaphoreType.DMA((3,)),
        ],
        compiler_params=params,
    )(
        table, labels, slots, patch_embed, positions, classifier, client_in, client_down,
        *in_pieces, *down_pieces,
    )
    losses, gclass = res[:2]
    packs = res[2:5]
    parts_in = list(res[5 : 5 + group])
    parts_down = list(res[5 + group :])

    half = group // 2
    while half:
        bit = half.bit_length() - 1
        parts_in = [
            parts_in[i].astype(F32) + flip(parts_in[i + half].astype(BF), bit).astype(F32)
            for i in range(half)
        ]
        parts_down = [
            parts_down[i].astype(F32) + flip(parts_down[i + half].astype(BF), bit).astype(F32)
            for i in range(half)
        ]
        half //= 2
    gsum = gclass.astype(F32)
    for bit in range(bits):
        gsum = gsum + flip(gsum.astype(BF), bit).astype(F32)
    grad_class = lax.dynamic_slice_in_dim(gsum, rank * rows_in, rows_in, 0)

    steps = bits_of(n)
    sums = pl.pallas_call(
        functools.partial(reduce_kernel, n),
        out_shape=[shape((r, width), F32) for r in tall],
        in_specs=[vmem()] * 3,
        out_specs=[vmem()] * 3,
        scratch_shapes=[
            pltpu.VMEM((n >> (t + 1), r, width), BF) for r in tall for t in range(steps)
        ]
        + [pltpu.VMEM((n >> (t + 1), r, width), BF) for r in tall for t in range(steps - 1)]
        + [
            pltpu.SemaphoreType.DMA((3, steps)),
            pltpu.SemaphoreType.DMA((3, steps)),
        ],
        compiler_params=pltpu.CompilerParams(
            collective_id=2, has_side_effects=True, vmem_limit_bytes=VMEM_LIMIT
        ),
    )(*packs)
    own = width // n
    extra = r_in - head
    grad_in = jnp.concatenate([sums[0], sums[1][:extra]], axis=0).T
    down = jnp.concatenate([sums[1][extra:], sums[2]], axis=0)
    down = down.reshape(ff // width + 1, PAD, width)[:, :own]
    grad_down = down[:-1].transpose(0, 2, 1).reshape(ff, own)
    last = down[-1].T
    return (
        losses,
        last[:patch],
        last[width - LANES : width - LANES + TOK],
        grad_in,
        grad_down,
        parts_in[0],
        parts_down[0],
        grad_class,
    )


def solution(mesh):
    whole = P()
    in_specs = (
        P("client", None), whole, whole, whole, whole, whole, whole,
        P(None, "client", None), P(None, "client", None), whole,
    )
    out_specs = (
        P("client", None), P(None, "client"), P(None, "client"), P(None, "client"),
        P(None, "client"), P(None, "client", None), P(None, "client", None), P("client", None),
    )
    return jax.shard_map(
        per_device, mesh=mesh, in_specs=in_specs, out_specs=out_specs, check_vma=False
    )
```

```python
import functools
import math

import jax
import jax.numpy as jnp
from jax import lax
from jax.experimental import pallas as pl
from jax.experimental.pallas import tpu as pltpu
from jax.sharding import PartitionSpec as P

HEADS = 6
TOK = 16
IMG = 8
SHARDS = 16
SLOTS = 2
PLANE = 4
EPSILON = 1e-06
LANES = 128
PAD = 16
BF = jnp.bfloat16
F32 = jnp.float32
HIGH = lax.Precision.HIGHEST
GELU_C = math.sqrt(2.0 / math.pi)
VMEM_LIMIT = 60 * 1024 * 1024
MESH = pl.DeviceIdType.MESH


def mm(a, b, precision=None):
    return lax.dot_general(
        a, b, (((1,), (0,)), ((), ())), precision=precision, preferred_element_type=F32
    )


def mm_nt(a, b, precision=None):
    return lax.dot_general(
        a, b, (((1,), (1,)), ((), ())), precision=precision, preferred_element_type=F32
    )


def mm_tn(a, b):
    return lax.dot_general(a, b, (((0,), (0,)), ((), ())), preferred_element_type=F32)


def norm(v):
    centre = v - jnp.mean(v, axis=-1, keepdims=True)
    scale = lax.rsqrt(jnp.mean(centre * centre, axis=-1, keepdims=True) + EPSILON)
    return centre * scale, scale


def norm_back(normed, scale, grad):
    return scale * (
        grad
        - jnp.mean(grad, axis=-1, keepdims=True)
        - normed * jnp.mean(grad * normed, axis=-1, keepdims=True)
    )


def gelu_both(v):
    sq = v * v
    t = jnp.tanh(v * (GELU_C + (GELU_C * 0.044715) * sq))
    half = 0.5 + 0.5 * t
    slope = half + (0.5 * v) * (1.0 - t * t) * (GELU_C + (GELU_C * 0.134145) * sq)
    return v * half, slope


def image_mask(per):
    row = lax.broadcasted_iota(jnp.int32, (per * LANES, LANES), 0) % LANES
    col = lax.broadcasted_iota(jnp.int32, (per * LANES, LANES), 1)
    return row // TOK == col // TOK


def lane_masks(head_dim):
    lane = lax.broadcasted_iota(jnp.int32, (LANES, LANES), 1)
    return [lane // head_dim == h for h in range(LANES // head_dim)]


def stack(value, keeps):
    return jnp.concatenate([jnp.where(k, value, jnp.zeros_like(value)) for k in keeps], axis=0)


def widen(value, per):
    return jnp.concatenate(
        [value[h * LANES : (h + 1) * LANES] for h in range(per)], axis=1
    )


def attend(qkv_ref, probs_ref, att_ref, width):
    rows = qkv_ref.shape[0]
    head_dim = width // HEADS
    per = LANES // head_dim
    inside = image_mask(per)
    keeps = lane_masks(head_dim)
    for group in range(rows // LANES):
        r = slice(group * LANES, (group + 1) * LANES)
        for pair in range(width // LANES):
            lo = pair * LANES
            q = qkv_ref[r, lo : lo + LANES]
            k = qkv_ref[r, width + lo : width + lo + LANES]
            v = qkv_ref[r, 2 * width + lo : 2 * width + lo + LANES]
            s = jnp.where(inside, mm_nt(stack(q, keeps), k), -1e30)
            e = jnp.exp(s - jnp.max(s, axis=-1, keepdims=True))
            p = (e * (1.0 / jnp.sum(e, axis=-1, keepdims=True))).astype(BF)
            probs_ref[group * (width // LANES) + pair] = p
            att_ref[r, lo : lo + LANES] = mm(widen(p, per), stack(v, keeps)).astype(BF)


def attend_back(grad, qkv_ref, probs_ref, dqkv_ref, width):
    rows = qkv_ref.shape[0]
    head_dim = width // HEADS
    per = LANES // head_dim
    keeps = lane_masks(head_dim)
    for group in range(rows // LANES):
        r = slice(group * LANES, (group + 1) * LANES)
        for pair in range(width // LANES):
            lo = pair * LANES
            q = qkv_ref[r, lo : lo + LANES]
            k = qkv_ref[r, width + lo : width + lo + LANES]
            v = qkv_ref[r, 2 * width + lo : 2 * width + lo + LANES]
            go = stack(grad[r, lo : lo + LANES].astype(BF), keeps)
            p = probs_ref[group * (width // LANES) + pair]
            dp = mm_nt(go, v)
            dv = mm_tn(p, go)
            pf = p.astype(F32)
            ds = (pf * (dp - jnp.sum(pf * dp, axis=-1, keepdims=True))).astype(BF)
            dq = mm(widen(ds, per), stack(k, keeps)) * (1.0 / math.sqrt(head_dim))
            dk = mm_tn(ds, stack(q, keeps))
            dqkv_ref[r, lo : lo + LANES] = dq.astype(BF)
            dqkv_ref[r, width + lo : width + lo + LANES] = dk.astype(BF)
            dqkv_ref[r, 2 * width + lo : 2 * width + lo + LANES] = dv.astype(BF)


def block_forward(x, w_ref, d_ref, first, qkv_ref, probs_ref, att_ref, second, h_ref, slope_ref):
    width = x.shape[1]
    ff = d_ref.shape[0]
    u, scale = norm(x)
    u = u.astype(BF)
    first[0][...] = u
    first[1][...] = scale
    for part in range(3):
        value = mm(u, w_ref[:, part * width : (part + 1) * width])
        if part == 0:
            value = value * (1.0 / math.sqrt(width // HEADS))
        qkv_ref[:, part * width : (part + 1) * width] = value.astype(BF)
    attend(qkv_ref, probs_ref, att_ref, width)
    y = x + mm(att_ref[...], w_ref[:, 3 * width : 4 * width])
    u, scale = norm(y)
    u = u.astype(BF)
    second[0][...] = u
    second[1][...] = scale
    for lo in range(0, ff, width):
        value, slope = gelu_both(mm(u, w_ref[:, 4 * width + lo : 5 * width + lo]))
        h_ref[:, lo : lo + width] = value.astype(BF)
        slope_ref[:, lo : lo + width] = slope.astype(BF)
    return y + mm(h_ref[...], d_ref[...])


def block_backward(
    g, w_ref, d_ref, first, qkv_ref, probs_ref, att_ref, second, h_ref, slope_ref, dqkv_ref,
    put_in, put_down, after=lambda stage: None,
):
    width = g.shape[1]
    ff = d_ref.shape[0]
    gb = g.astype(BF)
    put_down(h_ref, gb)
    after(0)
    for lo in range(0, ff, width):
        slope = slope_ref[:, lo : lo + width].astype(F32)
        slope_ref[:, lo : lo + width] = (mm_nt(gb, d_ref[lo : lo + width, :]) * slope).astype(BF)
    put_in(4 * width, second[0], slope_ref)
    after(1)
    dy = g + norm_back(
        second[0][...].astype(F32), second[1][...], mm_nt(slope_ref[...], w_ref[:, 4 * width :])
    )
    gb = dy.astype(BF)
    dqkv_ref[:, :width] = gb
    put_in(3 * width, att_ref, dqkv_ref.at[:, :width])
    after(2)
    attend_back(
        mm_nt(gb, w_ref[:, 3 * width : 4 * width]), qkv_ref, probs_ref, dqkv_ref, width
    )
    after(3)
    put_in(0, first[0], dqkv_ref)
    after(4)
    return dy + norm_back(
        first[0][...].astype(F32), first[1][...], mm_nt(dqkv_ref[...], w_ref[:, : 3 * width])
    )


def bits_of(n):
    return n.bit_length() - 1


def place_of(device, order):
    index = 0
    for bit in order:
        index = index * 2 + (device >> bit & 1)
    return index


def pad_of(own):
    return (own + 7) // 8 * 8


def chain_plan(n, r_in, blocks, pad):
    steps = bits_of(n)
    rest = list(range(1, steps))
    far = rest[-2:]
    near = rest[:-2]
    low = near[: len(near) // 2]
    high = near[len(near) // 2 :]
    first = [0] + low + high + far
    second = [0] + high + low + far
    third = [0] + far + low + high
    top = (r_in // 2 + PAD - 1) // PAD * PAD
    half = blocks // 2 * pad
    return [
        (half, first), (blocks * pad - half, second),
        (top, first[:-1]), (r_in - top, second[:-1]),
        (top, first[:-1]), (r_in - top, second[:-1]),
        (pad, third),
    ]


DOWN, UPPER, LOWER, LAST = 0, 2, 4, 6


def step_kernel(n, group, layers, per_image, capacity, classes, plan, *refs):
    (
        assign_hbm, label_hbm, turned_hbm, embed_hbm, pos_hbm, class_hbm,
        cin_hbm, cdown_hbm, sin_hbm, sdown_hbm,
    ) = refs[:10]
    refs = refs[10:]
    loss_ref, gclass_ref, gin_sum, gdown_sum, cin_sum, down_first, down_second, last_sum = refs[:8]
    refs = refs[8:]
    (
        assign_ref, label_ref, turned_ref, embed_ref, pos_ref, class_ref,
        patch_ref, column, pack, got_slots, slots_ref,
        first_u, first_s, qkv, probs, att, second_u, second_s, hidden,
        slope, dqkv, gcur,
        gclass_own, gclass_got, joined, joined_got,
    ) = refs[:26]
    refs = refs[26:]
    wbuf, dbuf, refs = refs[: layers + 1], refs[layers + 1 : 2 * layers + 2], refs[2 * layers + 2 :]
    gin, gdown, refs = refs[:layers], refs[layers : 2 * layers], refs[2 * layers :]
    gin_got, gdown_got, refs = refs[:layers], refs[layers : 2 * layers], refs[2 * layers :]
    chains = len(plan)
    packs, refs = refs[:chains], refs[chains:]
    got, held = [], []
    for rows, order in plan:
        count = len(order)
        got.append(refs[:count])
        held.append(refs[count : 2 * count - 1])
        refs = refs[2 * count - 1 :]
    (
        load_sem, own_sem, near_send, near_recv, far_send, far_recv, flat_send, flat_recv,
        w_send, w_recv, g_send, g_recv, c_send, c_recv, r_send, r_recv, j_send, j_recv,
    ) = refs
    steps = bits_of(n)
    me = lax.axis_index("client")
    rank = me % group
    shard = me // group
    line = shard // PLANE
    spot = shard % PLANE
    rows_in = sin_hbm.shape[1]
    rows_down = sdown_hbm.shape[1]
    rows, width = gcur.shape
    ff = dbuf[0].shape[0]

    loads = [
        pltpu.make_async_copy(source, target, load_sem.at[i])
        for i, (source, target) in enumerate([
            (turned_hbm, turned_ref), (assign_hbm, assign_ref), (label_hbm, label_ref),
            (embed_hbm, embed_ref), (pos_hbm, pos_ref), (class_hbm, class_ref),
            (cin_hbm, wbuf[0]), (cdown_hbm, dbuf[0]),
        ])
    ]
    for c in loads:
        c.start()

    def own_in(layer):
        return pltpu.make_async_copy(
            sin_hbm.at[layer],
            wbuf[layer + 1].at[pl.ds(rank * rows_in, rows_in)],
            own_sem.at[layer, 0],
        )

    def own_down(layer):
        return pltpu.make_async_copy(
            sdown_hbm.at[layer],
            dbuf[layer + 1].at[pl.ds(rank * rows_down, rows_down)],
            own_sem.at[layer, 1],
        )

    def near_peer(i):
        return shard * group + lax.rem(rank + i, group)

    def far_peer(i):
        return (lax.rem(line + i, PLANE) * PLANE + spot) * group + rank

    def flat_peer(i):
        return (line * PLANE + lax.rem(spot + i, PLANE)) * group + rank

    def remote(source, target, send, recv, peer):
        return pltpu.make_async_remote_copy(
            src_ref=source, dst_ref=target, send_sem=send, recv_sem=recv,
            device_id=(peer,), device_id_type=MESH,
        )

    def near(i):
        to = lax.rem(rank + i, group)
        return remote(
            patch_ref.at[to], column.at[line, rank], near_send.at[i], near_recv.at[i], near_peer(i)
        )

    def far(i, j):
        if j == 0:
            source, member = patch_ref.at[rank], rank
        else:
            member = lax.rem(rank + group - j, group)
            source = column.at[line, member]
        return remote(
            source, column.at[line, member], far_send.at[i, j], far_recv.at[i, j], far_peer(i)
        )

    def flat(i):
        return remote(
            pack.at[i], got_slots.at[spot], flat_send.at[i], flat_recv.at[i], flat_peer(i)
        )

    def weight_in(layer, i):
        return remote(
            sin_hbm.at[layer],
            wbuf[layer + 1].at[pl.ds(rank * rows_in, rows_in)],
            w_send.at[layer, i, 0], w_recv.at[layer, i, 0], near_peer(i),
        )

    def weight_down(layer, i):
        return remote(
            sdown_hbm.at[layer],
            dbuf[layer + 1].at[pl.ds(rank * rows_down, rows_down)],
            w_send.at[layer, i, 1], w_recv.at[layer, i, 1], near_peer(i),
        )

    def grad_in(layer, i):
        to = lax.rem(rank + i, group)
        return remote(
            gin[layer].at[pl.ds(to * rows_in, rows_in)],
            gin_got[layer].at[i - 1], g_send.at[layer, i, 0], g_recv.at[layer, i, 0], near_peer(i),
        )

    def grad_down(layer, i):
        to = lax.rem(rank + i, group)
        return remote(
            gdown[layer].at[pl.ds(to * rows_down, rows_down)],
            gdown_got[layer].at[i - 1], g_send.at[layer, i, 1], g_recv.at[layer, i, 1],
            near_peer(i),
        )

    def grad_class(i):
        return remote(gclass_own, gclass_got.at[i - 1], c_send.at[i], c_recv.at[i], near_peer(i))

    barrier = pltpu.get_barrier_semaphore()
    peers = [near_peer(i) for i in range(1, group)]
    peers += [far_peer(i) for i in range(1, PLANE)]
    peers += [flat_peer(i) for i in range(1, PLANE)]
    for peer in peers:
        pl.semaphore_signal(barrier, inc=1, device_id=(peer,), device_id_type=MESH)
    for layer in range(layers):
        own_in(layer).start()
        own_down(layer).start()
    loads[0].wait()
    patch_ref[...] = turned_ref[...].astype(F32).T.astype(BF).reshape(patch_ref.shape)
    pl.semaphore_wait(barrier, len(peers))

    for i in range(1, group):
        near(i).start()
    for i in range(1, PLANE):
        far(i, 0).start()
    for layer in range(layers):
        for i in range(1, group):
            weight_in(layer, i).start()
            weight_down(layer, i).start()
    for j in range(1, group):
        near(j).wait_recv()
        for i in range(1, PLANE):
            far(i, j).start()
    column[line, rank] = patch_ref[rank]

    targets = [line * PLANE + lax.rem(spot + i, PLANE) for i in range(PLANE)]
    loads[1].wait()
    loads[2].wait()

    def scan(c, carry):
        there = assign_ref[c]
        out = []
        for i in range(PLANE):
            count, slots = carry[i]
            hit = there == targets[i]
            slots = tuple(
                jnp.where(hit & (count == k), c, slots[k]) for k in range(capacity)
            )
            out.append((count + jnp.where(hit, 1, 0), slots))
        return tuple(out)

    zero = jnp.int32(0)
    table = lax.fori_loop(
        0, n, scan, tuple((zero, tuple(zero for _ in range(capacity))) for _ in range(PLANE))
    )
    filled, slots = table[0]
    images = capacity * per_image
    row = lax.broadcasted_iota(jnp.int32, (images, classes), 0)
    lane = lax.broadcasted_iota(jnp.int32, (images, classes), 1)
    want = jnp.full((images, classes), -1, jnp.int32)
    for k in range(capacity):
        base = slots[k] * (group * per_image) + rank * per_image
        for j in range(per_image):
            lab = jnp.where(k < filled, label_ref[base + j], -1)
            want = jnp.where(row == k * per_image + j, lab, want)
    hot = (lane == want).astype(F32)
    full = (want[:, :1] >= 0).astype(F32)
    loads[5].wait()
    every = class_ref[...].astype(F32)
    chosen = lax.broadcasted_iota(jnp.int32, every.shape, 1) == shard
    cls = jnp.sum(jnp.where(chosen, every, 0.0), axis=1).astype(BF)

    for i in range(1, PLANE):
        for j in range(group):
            far(i, j).wait_recv()

    def pick(c):
        home = c // group
        return column[home // PLANE, c % group]

    for i in range(1, PLANE):
        for k in range(capacity):
            pack[i, k] = pick(table[i][1][k])
        flat(i).start()
    for k in range(capacity):
        got_slots[spot, k] = pick(slots[k])
    for c in (3, 4, 6, 7):
        loads[c].wait()
    for i in range(1, PLANE):
        flat(i).wait_recv()
    piece = patch_ref.shape[1]
    for k in range(capacity):
        home = slots[k] // group
        slots_ref[k * piece : (k + 1) * piece, :] = got_slots[home % PLANE, k]

    x = mm(slots_ref[...], embed_ref[...])
    pos = pos_ref[...].astype(F32)
    gcur[...] = x + jnp.concatenate([pos] * (rows // TOK), axis=0)

    def saved(layer):
        return (
            (first_u.at[layer], first_s.at[layer]), qkv.at[layer], probs.at[layer], att.at[layer],
            (second_u.at[layer], second_s.at[layer]), hidden.at[layer], slope.at[layer],
        )

    for layer in range(layers + 1):
        if layer > 0:
            own_in(layer - 1).wait()
            own_down(layer - 1).wait()
            for i in range(1, group):
                weight_in(layer - 1, i).wait_recv()
                weight_down(layer - 1, i).wait_recv()

        out = block_forward(gcur[...], wbuf[layer], dbuf[layer], *saved(layer))
        gcur[...] = out if layer else out.astype(BF).astype(F32)

    pool = (
        lax.broadcasted_iota(jnp.int32, (images, rows), 1) // TOK
        == lax.broadcasted_iota(jnp.int32, (images, rows), 0)
    ).astype(F32) * (1.0 / TOK)
    unpool = (
        lax.broadcasted_iota(jnp.int32, (rows, images), 0) // TOK
        == lax.broadcasted_iota(jnp.int32, (rows, images), 1)
    ).astype(F32) * (1.0 / TOK)
    u, scale = norm(mm(pool, gcur[...], HIGH))
    pooled = u.astype(BF)
    logits = mm_nt(pooled, cls)
    top = jnp.max(logits, axis=-1, keepdims=True)
    e = jnp.exp(logits - top)
    total = jnp.sum(e, axis=-1, keepdims=True)
    loss = (
        jnp.log(total) + top - jnp.sum(jnp.where(lane == want, logits, 0.0), axis=-1, keepdims=True)
    ) * full
    eye = (
        lax.broadcasted_iota(jnp.int32, (images, images), 0)
        == lax.broadcasted_iota(jnp.int32, (images, images), 1)
    )
    loss_ref[...] = jnp.sum(jnp.where(eye, loss, 0.0), axis=0, keepdims=True)
    dlog = ((e / total - hot) * full).astype(BF)
    gclass_own[...] = mm_tn(dlog, pooled).astype(BF)
    for i in range(1, group):
        grad_class(i).start()
    dpool = norm_back(u, scale, mm(dlog, cls))
    gcur[...] = mm(unpool, dpool, HIGH)

    for layer in reversed(range(layers)):
        def put_in(start, lhs, rhs, layer=layer):
            for c in range(0, rhs.shape[1], width):
                gin[layer][:, start + c : start + c + width] = mm_tn(
                    lhs[...], rhs[:, c : c + width]
                ).astype(BF)

        def put_down(h, gb, layer=layer):
            for c in range(0, ff, width):
                gdown[layer][c : c + width] = mm_tn(h[:, c : c + width], gb).astype(BF)

        deep = layer + 1
        gcur[...] = block_backward(
            gcur[...], wbuf[deep], dbuf[deep], *saved(deep), dqkv, put_in, put_down,
        )
        for i in range(1, group):
            grad_down(layer, i).start()
            grad_in(layer, i).start()

    def peer_of(bit):
        return me + (1 << bit) - 2 * (1 << bit) * (me // (1 << bit) % 2)

    def mine(bit):
        return me // (1 << bit) % 2

    def source(c, t):
        return packs[c] if t == 0 else held[c][t - 1]

    def size_at(c, t):
        return packs[c].shape[0] >> (t + 1)

    def copy(c, t):
        bit = plan[c][1][t]
        half = size_at(c, t)
        return remote(
            source(c, t).at[pl.ds((1 - mine(bit)) * half, half)], got[c][t],
            r_send.at[c, t], r_recv.at[c, t], peer_of(bit),
        )

    def join(c):
        bit = steps - 1
        take = plan[UPPER + c][0]
        return remote(
            joined.at[c, 1 - mine(bit), pl.ds(0, take)], joined_got.at[c, pl.ds(0, take)],
            j_send.at[c], j_recv.at[c], peer_of(bit),
        )

    def store_final(c, value):
        if c == LAST:
            last_sum[...] = value
        elif c == DOWN:
            down_first[...] = value
        elif c == DOWN + 1:
            down_second[...] = value
        else:
            side = 1 if c < LOWER else 0
            joined[c % 2, side, : value.shape[0]] = value.astype(BF)

    progress = [0] * chains

    def advance(c):
        t = progress[c]
        count = len(plan[c][1])
        if t >= count:
            return
        progress[c] = t + 1
        half = size_at(c, t)
        copy(c, t).wait_recv()
        first = mine(plan[c][1][t]) * half
        if t == count - 1:
            store_final(c, source(c, t)[first].astype(F32) + got[c][t][0].astype(F32))
            return

        def add(e, carry):
            held[c][t][e] = (
                source(c, t)[first + e].astype(F32) + got[c][t][e].astype(F32)
            ).astype(BF)
            return carry

        lax.fori_loop(0, half, add, 0)
        copy(c, t + 1).start()

    per_dev = wbuf[0].shape[1] // n
    cols = width // n
    pad = pad_of(cols)
    src = lax.broadcasted_iota(jnp.int32, (width, n * pad), 0)
    dst = lax.broadcasted_iota(jnp.int32, (width, n * pad), 1)
    spread_to = ((dst // pad == src // cols) & (dst % pad == src % cols)).astype(F32).astype(BF)
    tok = (
        lax.broadcasted_iota(jnp.int32, (rows, LANES), 0) % TOK
        == lax.broadcasted_iota(jnp.int32, (rows, LANES), 1)
    ).astype(F32).astype(BF)

    def put_in(start, lhs, rhs):
        base = UPPER if start >= 4 * width else LOWER
        for c in range(0, rhs.shape[1], width):
            part = mm_tn(rhs[:, c : c + width], lhs[...]).astype(BF)
            first = (start + c) // per_dev
            for j in range(width // per_dev):
                lo = j * per_dev
                for piece_at in range(2):
                    take, order = plan[base + piece_at]
                    packs[base + piece_at][place_of(first + j, order)] = part[lo : lo + take]
                    lo += take

    def put_down(h, gb):
        spread = mm(gb, spread_to).astype(BF)
        for q in range(ff // width):
            part = mm_tn(spread, h[:, q * width : (q + 1) * width]).astype(BF)
            c = DOWN if q * pad < plan[DOWN][0] else DOWN + 1
            lo = q * pad if c == DOWN else q * pad - plan[DOWN][0]
            for j in range(n):
                packs[c][place_of(j, plan[c][1]), lo : lo + pad] = part[j * pad : (j + 1) * pad]

    def after(stage):
        if stage == 0:
            copy(DOWN, 0).start()
            copy(DOWN + 1, 0).start()
        elif stage == 1:
            copy(UPPER, 0).start()
            copy(UPPER + 1, 0).start()
            advance(DOWN)
            advance(DOWN + 1)
        elif stage == 2:
            advance(UPPER)
            advance(UPPER + 1)
        elif stage == 3:
            advance(DOWN)
            advance(DOWN + 1)
        else:
            copy(LOWER, 0).start()
            copy(LOWER + 1, 0).start()

    dx = block_backward(
        gcur[...].astype(BF).astype(F32), wbuf[0], dbuf[0], *saved(0), dqkv,
        put_in, put_down, after,
    )
    spread = mm(dx.astype(BF), spread_to).astype(BF)
    patch = slots_ref.shape[1]
    embed_part = mm_tn(spread, slots_ref[...]).astype(BF)
    pos_part = mm_tn(spread, tok).astype(BF)
    for j in range(n):
        at = place_of(j, plan[LAST][1])
        packs[LAST][at, :, :patch] = embed_part[j * pad : (j + 1) * pad]
        packs[LAST][at, :, patch : width - LANES] = jnp.zeros((pad, width - LANES - patch), BF)
        packs[LAST][at, :, width - LANES :] = pos_part[j * pad : (j + 1) * pad]
    copy(LAST, 0).start()

    def add_layer(layer):
        for i in range(1, group):
            grad_down(layer, i).wait_recv()
            grad_in(layer, i).wait_recv()
        start = rank * rows_in
        whole = gin[layer][pl.ds(start, rows_in)].astype(F32)
        for i in range(1, group):
            whole = whole + gin_got[layer][i - 1].astype(F32)
        gin_sum[layer] = whole.astype(BF)
        start = rank * rows_down
        whole = gdown[layer][pl.ds(start, rows_down)].astype(F32)
        for i in range(1, group):
            whole = whole + gdown_got[layer][i - 1].astype(F32)
        gdown_sum[layer] = whole.astype(BF)

    rounds = 0
    while any(progress[c] < len(plan[c][1]) for c in range(chains)):
        for c in (LOWER, LOWER + 1, UPPER, UPPER + 1, LAST, DOWN, DOWN + 1):
            done = progress[c] == len(plan[c][1])
            advance(c)
            if LOWER <= c < LAST and not done and progress[c] == len(plan[c][1]):
                other = c - LOWER + UPPER
                while progress[other] < len(plan[other][1]):
                    advance(other)
                join(c - LOWER).start()
        if rounds < layers:
            add_layer(layers - 1 - rounds)
        rounds += 1
    for i in range(1, group):
        grad_class(i).wait_recv()
    both = gclass_own[...].astype(F32)
    for i in range(1, group):
        both = both + gclass_got[i - 1].astype(F32)
    kept = both[:, :rows_in]
    for i in range(1, group):
        kept = jnp.where(rank == i, both[:, i * rows_in : (i + 1) * rows_in], kept)
    gclass_ref[...] = kept
    lo = 0
    for c in range(2):
        join(c).wait_recv()
        take = plan[UPPER + c][0]
        cin_sum[lo : lo + take, :] = (
            joined[c, mine(steps - 1), :take].astype(F32) + joined_got[c, :take].astype(F32)
        )
        lo += take

    for i in range(1, group):
        near(i).wait_send()
        grad_class(i).wait_send()
        for layer in range(layers):
            weight_in(layer, i).wait_send()
            weight_down(layer, i).wait_send()
            grad_in(layer, i).wait_send()
            grad_down(layer, i).wait_send()
    for i in range(1, PLANE):
        flat(i).wait_send()
        for j in range(group):
            far(i, j).wait_send()
    for c in range(chains):
        for t in range(len(plan[c][1])):
            copy(c, t).wait_send()
    for c in range(2):
        join(c).wait_send()


def finish_kernel(
    near_in, near_down, class_ref, loss_in, cin_sum, down_first, down_second, last_sum,
    gin_ref, gdown_ref, gclass_ref, loss_ref, cin_ref, cdown_ref, embed_ref, pos_ref,
):
    gin_ref[...] = near_in[...].astype(F32)
    gdown_ref[...] = near_down[...].astype(F32)

    @pl.when((pl.program_id(0) == 0) & (pl.program_id(1) == 0))
    def _():
        gclass_ref[...] = class_ref[...]
        loss_ref[...] = loss_in[...]
        cin_ref[...] = cin_sum[...]
        own, width = cdown_ref.shape[0], cin_sum.shape[1]
        pad = pad_of(own)
        q = 0
        for part in (down_first, down_second):
            for lo in range(0, part.shape[0], pad):
                cdown_ref[:, q * width : (q + 1) * width] = part[lo : lo + pad, :][:own]
                q += 1
        last = last_sum[...]
        embed_ref[...] = last[:own, : embed_ref.shape[1]]
        pos_ref[...] = last[:, width - LANES :].T[:TOK, :own]


def vmem():
    return pl.BlockSpec(memory_space=pltpu.VMEM)


def hbm():
    return pl.BlockSpec(memory_space=pltpu.HBM)


def shape(dims, kind):
    return jax.ShapeDtypeStruct(dims, kind)


def per_device(
    patches, labels, assign, patch_embed, positions, client_in, client_down,
    server_in, server_down, classifier,
):
    n = lax.axis_size("client")
    group = n // SHARDS
    rows = patches.shape[0]
    patch = patches.shape[1]
    width = client_in.shape[0]
    cols = client_in.shape[1]
    ff = client_down.shape[0]
    layers = server_in.shape[0]
    rows_in = server_in.shape[1]
    rows_down = server_down.shape[1]
    classes = classifier.shape[2]
    piece = rows // group
    per_image = IMG // group
    capacity = SLOTS * group
    s_rows = capacity * piece
    r_in = cols // n
    own = width // n
    steps = bits_of(n)
    pad = pad_of(own)
    plan = chain_plan(n, r_in, ff // width, pad)
    shards = classifier.shape[0]
    per = LANES // (width // HEADS)
    spaces = [
        ((s_rows, width), BF),
        ((s_rows, 1), F32),
        ((s_rows, 3 * width), BF),
        ((s_rows // LANES * (width // LANES), per * LANES, LANES), BF),
        ((s_rows, width), BF),
        ((s_rows, width), BF),
        ((s_rows, 1), F32),
        ((s_rows, ff), BF),
        ((s_rows, ff), BF),
    ]
    scratch = [
        pltpu.SMEM((n,), jnp.int32),
        pltpu.SMEM((n * IMG,), jnp.int32),
        pltpu.VMEM((patch, rows), BF),
        pltpu.VMEM((patch, width), BF),
        pltpu.VMEM((TOK, width), BF),
        pltpu.VMEM((classes, shards, width), BF),
        pltpu.VMEM((group, piece, patch), BF),
        pltpu.VMEM((PLANE, group, piece, patch), BF),
        pltpu.VMEM((PLANE, capacity, piece, patch), BF),
        pltpu.VMEM((PLANE, capacity, piece, patch), BF),
        pltpu.VMEM((s_rows, patch), BF),
    ]
    scratch += [pltpu.VMEM((layers + 1,) + dims, kind) for dims, kind in spaces]
    scratch += [
        pltpu.VMEM((s_rows, 3 * width), BF),
        pltpu.VMEM((s_rows, width), F32),
        pltpu.VMEM((classes, width), BF),
        pltpu.VMEM((group - 1, classes, width), BF),
        pltpu.VMEM((2, 2, plan[UPPER][0], width), BF),
        pltpu.VMEM((2, plan[UPPER][0], width), BF),
    ]
    scratch += [pltpu.VMEM((width, cols), BF)] * (layers + 1)
    scratch += [pltpu.VMEM((ff, width), BF)] * (layers + 1)
    scratch += [pltpu.VMEM((width, cols), BF)] * layers
    scratch += [pltpu.VMEM((ff, width), BF)] * layers
    scratch += [pltpu.VMEM((group - 1, rows_in, cols), BF)] * layers
    scratch += [pltpu.VMEM((group - 1, rows_down, width), BF)] * layers
    scratch += [pltpu.VMEM((1 << len(order), r, width), BF) for r, order in plan]
    for r, order in plan:
        count = len(order)
        scratch += [pltpu.VMEM((1 << (count - 1 - t), r, width), BF) for t in range(count)]
        scratch += [pltpu.VMEM((1 << (count - 1 - t), r, width), BF) for t in range(count - 1)]
    scratch += [
        pltpu.SemaphoreType.DMA(dims)
        for dims in [
            (8,), (layers, 2), (group,), (group,), (PLANE, group), (PLANE, group), (PLANE,),
            (PLANE,), (layers, group, 2), (layers, group, 2), (layers, group, 2),
            (layers, group, 2), (group,), (group,), (len(plan), steps), (len(plan), steps),
            (2,), (2,),
        ]
    ]
    found = pl.pallas_call(
        functools.partial(step_kernel, n, group, layers, per_image, capacity, classes, plan),
        out_shape=[
            shape((1, capacity * per_image), F32),
            shape((classes, rows_in), F32),
            shape((layers, rows_in, cols), BF),
            shape((layers, rows_down, width), BF),
            shape((r_in, width), F32),
            shape((plan[DOWN][0], width), F32),
            shape((plan[DOWN + 1][0], width), F32),
            shape((pad, width), F32),
        ],
        in_specs=[hbm()] * 10,
        out_specs=[vmem()] * 8,
        scratch_shapes=scratch,
        compiler_params=pltpu.CompilerParams(
            collective_id=1, has_side_effects=True, vmem_limit_bytes=VMEM_LIMIT
        ),
    )(
        assign.reshape(n), labels, patches.T, patch_embed, positions,
        classifier.transpose(2, 0, 1), client_in, client_down, server_in, server_down,
    )
    loss, gclass, gin, gdown, *sums = found
    cuts = 4 if rows_in % (4 * PAD) == 0 else 1

    def tile(r, c):
        return pl.BlockSpec((1, r // cuts, c), lambda i, j: (i, j, 0))

    def whole(*dims):
        return pl.BlockSpec(dims, lambda i, j: (0, 0))

    gin, gdown, gclass, loss, cin, cdown, embed, pos = pl.pallas_call(
        finish_kernel,
        grid=(layers, cuts),
        out_shape=[
            shape((layers, rows_in, cols), F32),
            shape((layers, rows_down, width), F32),
            shape((classes, rows_in), F32),
            shape((1, capacity * per_image), F32),
            shape((r_in, width), F32),
            shape((own, ff), F32),
            shape((own, patch), F32),
            shape((TOK, own), F32),
        ],
        in_specs=[
            tile(rows_in, cols),
            tile(rows_down, width),
            whole(classes, rows_in),
            whole(1, capacity * per_image),
        ]
        + [whole(*v.shape) for v in sums],
        out_specs=[
            tile(rows_in, cols),
            tile(rows_down, width),
            whole(classes, rows_in),
            whole(1, capacity * per_image),
            whole(r_in, width),
            whole(own, ff),
            whole(own, patch),
            whole(TOK, own),
        ],
        compiler_params=pltpu.CompilerParams(
            dimension_semantics=("arbitrary", "arbitrary"), vmem_limit_bytes=24 * 1024 * 1024
        ),
    )(gin, gdown, gclass, loss, *sums)
    return loss, embed.T, pos, cin.T, cdown.T, gin, gdown, gclass.T


def solution(mesh):
    whole = P()
    in_specs = (
        P("client", None), whole, whole, whole, whole, whole, whole,
        P(None, "client", None), P(None, "client", None), whole,
    )
    out_specs = (
        P("client", None), P(None, "client"), P(None, "client"), P(None, "client"),
        P(None, "client"), P(None, "client", None), P(None, "client", None), P("client", None),
    )
    return jax.shard_map(
        per_device, mesh=mesh, in_specs=in_specs, out_specs=out_specs, check_vma=False
    )
```

```python
import functools
import math

import jax
import jax.numpy as jnp
from jax import lax
from jax.experimental import pallas as pl
from jax.experimental.pallas import tpu as pltpu
from jax.sharding import PartitionSpec as P

HEADS = 6
TOK = 16
IMG = 8
SHARDS = 16
SLOTS = 2
PLANE = 4
EPSILON = 1e-06
LANES = 128
PAD = 16
BF = jnp.bfloat16
F32 = jnp.float32
HIGH = lax.Precision.HIGHEST
GELU_C = math.sqrt(2.0 / math.pi)
VMEM_LIMIT = 60 * 1024 * 1024
MESH = pl.DeviceIdType.MESH


def mm(a, b, precision=None):
    return lax.dot_general(
        a, b, (((1,), (0,)), ((), ())), precision=precision, preferred_element_type=F32
    )


def mm_nt(a, b, precision=None):
    return lax.dot_general(
        a, b, (((1,), (1,)), ((), ())), precision=precision, preferred_element_type=F32
    )


def mm_tn(a, b):
    return lax.dot_general(a, b, (((0,), (0,)), ((), ())), preferred_element_type=F32)


def norm(v):
    centre = v - jnp.mean(v, axis=-1, keepdims=True)
    scale = lax.rsqrt(jnp.mean(centre * centre, axis=-1, keepdims=True) + EPSILON)
    return centre * scale, scale


def norm_back(normed, scale, grad):
    return scale * (
        grad
        - jnp.mean(grad, axis=-1, keepdims=True)
        - normed * jnp.mean(grad * normed, axis=-1, keepdims=True)
    )


def gelu_both(v):
    sq = v * v
    t = jnp.tanh(v * (GELU_C + (GELU_C * 0.044715) * sq))
    half = 0.5 + 0.5 * t
    slope = half + (0.5 * v) * (1.0 - t * t) * (GELU_C + (GELU_C * 0.134145) * sq)
    return v * half, slope


def image_mask(per):
    row = lax.broadcasted_iota(jnp.int32, (per * LANES, LANES), 0) % LANES
    col = lax.broadcasted_iota(jnp.int32, (per * LANES, LANES), 1)
    return row // TOK == col // TOK


def lane_masks(head_dim):
    lane = lax.broadcasted_iota(jnp.int32, (LANES, LANES), 1)
    return [lane // head_dim == h for h in range(LANES // head_dim)]


def stack(value, keeps):
    return jnp.concatenate([jnp.where(k, value, jnp.zeros_like(value)) for k in keeps], axis=0)


def widen(value, per):
    return jnp.concatenate(
        [value[h * LANES : (h + 1) * LANES] for h in range(per)], axis=1
    )


def attend(qkv_ref, probs_ref, att_ref, width):
    rows = qkv_ref.shape[0]
    head_dim = width // HEADS
    per = LANES // head_dim
    inside = image_mask(per)
    keeps = lane_masks(head_dim)
    for group in range(rows // LANES):
        r = slice(group * LANES, (group + 1) * LANES)
        for pair in range(width // LANES):
            lo = pair * LANES
            q = qkv_ref[r, lo : lo + LANES]
            k = qkv_ref[r, width + lo : width + lo + LANES]
            v = qkv_ref[r, 2 * width + lo : 2 * width + lo + LANES]
            s = jnp.where(inside, mm_nt(stack(q, keeps), k), -1e30)
            e = jnp.exp(s - jnp.max(s, axis=-1, keepdims=True))
            p = (e * (1.0 / jnp.sum(e, axis=-1, keepdims=True))).astype(BF)
            probs_ref[group * (width // LANES) + pair] = p
            att_ref[r, lo : lo + LANES] = mm(widen(p, per), stack(v, keeps)).astype(BF)


def attend_back(grad, qkv_ref, probs_ref, dqkv_ref, width):
    rows = qkv_ref.shape[0]
    head_dim = width // HEADS
    per = LANES // head_dim
    keeps = lane_masks(head_dim)
    for group in range(rows // LANES):
        r = slice(group * LANES, (group + 1) * LANES)
        for pair in range(width // LANES):
            lo = pair * LANES
            q = qkv_ref[r, lo : lo + LANES]
            k = qkv_ref[r, width + lo : width + lo + LANES]
            v = qkv_ref[r, 2 * width + lo : 2 * width + lo + LANES]
            go = stack(grad[r, lo : lo + LANES].astype(BF), keeps)
            p = probs_ref[group * (width // LANES) + pair]
            dp = mm_nt(go, v)
            dv = mm_tn(p, go)
            pf = p.astype(F32)
            ds = (pf * (dp - jnp.sum(pf * dp, axis=-1, keepdims=True))).astype(BF)
            dq = mm(widen(ds, per), stack(k, keeps)) * (1.0 / math.sqrt(head_dim))
            dk = mm_tn(ds, stack(q, keeps))
            dqkv_ref[r, lo : lo + LANES] = dq.astype(BF)
            dqkv_ref[r, width + lo : width + lo + LANES] = dk.astype(BF)
            dqkv_ref[r, 2 * width + lo : 2 * width + lo + LANES] = dv.astype(BF)


def block_forward(x, w_ref, d_ref, first, qkv_ref, probs_ref, att_ref, second, h_ref, slope_ref):
    width = x.shape[1]
    ff = d_ref.shape[0]
    u, scale = norm(x)
    u = u.astype(BF)
    first[0][...] = u
    first[1][...] = scale
    for part in range(3):
        value = mm(u, w_ref[:, part * width : (part + 1) * width])
        if part == 0:
            value = value * (1.0 / math.sqrt(width // HEADS))
        qkv_ref[:, part * width : (part + 1) * width] = value.astype(BF)
    attend(qkv_ref, probs_ref, att_ref, width)
    y = x + mm(att_ref[...], w_ref[:, 3 * width : 4 * width])
    u, scale = norm(y)
    u = u.astype(BF)
    second[0][...] = u
    second[1][...] = scale
    for lo in range(0, ff, width):
        value, slope = gelu_both(mm(u, w_ref[:, 4 * width + lo : 5 * width + lo]))
        h_ref[:, lo : lo + width] = value.astype(BF)
        slope_ref[:, lo : lo + width] = slope.astype(BF)
    return y + mm(h_ref[...], d_ref[...])


def block_backward(
    g, w_ref, d_ref, first, qkv_ref, probs_ref, att_ref, second, h_ref, slope_ref, dqkv_ref,
    put_in, put_down, after=lambda stage: None,
):
    width = g.shape[1]
    ff = d_ref.shape[0]
    gb = g.astype(BF)
    put_down(h_ref, gb)
    after(0)
    for lo in range(0, ff, width):
        slope = slope_ref[:, lo : lo + width].astype(F32)
        slope_ref[:, lo : lo + width] = (mm_nt(gb, d_ref[lo : lo + width, :]) * slope).astype(BF)
    put_in(4 * width, second[0], slope_ref)
    after(1)
    dy = g + norm_back(
        second[0][...].astype(F32), second[1][...], mm_nt(slope_ref[...], w_ref[:, 4 * width :])
    )
    gb = dy.astype(BF)
    dqkv_ref[:, :width] = gb
    put_in(3 * width, att_ref, dqkv_ref.at[:, :width])
    after(2)
    attend_back(
        mm_nt(gb, w_ref[:, 3 * width : 4 * width]), qkv_ref, probs_ref, dqkv_ref, width
    )
    after(3)
    put_in(0, first[0], dqkv_ref)
    after(4)
    return dy + norm_back(
        first[0][...].astype(F32), first[1][...], mm_nt(dqkv_ref[...], w_ref[:, : 3 * width])
    )


def bits_of(n):
    return n.bit_length() - 1


def place_of(device, order):
    index = 0
    for bit in order:
        index = index * 2 + (device >> bit & 1)
    return index


def pad_of(own):
    return (own + 7) // 8 * 8


def chain_plan(n, r_in, blocks, pad):
    steps = bits_of(n)
    rest = list(range(1, steps))
    far = rest[-2:]
    near = rest[:-2]
    low = near[: len(near) // 2]
    high = near[len(near) // 2 :]
    first = [0] + low + high + far
    second = [0] + high + low + far
    third = [0] + far + low + high
    top = (r_in // 2 + PAD - 1) // PAD * PAD
    return [
        (pad, first), (pad, second), ((blocks - 2) * pad, third),
        (top, first[:-1]), (r_in - top, second[:-1]),
        (top, first[:-1]), (r_in - top, second[:-1]),
        (pad, third),
    ]


DOWN, UPPER, LOWER, LAST = 0, 3, 5, 7


def layout_of(r_in, blocks, pad):
    sizes = [r_in] + [pad] * (blocks + 1) + [16, 8]
    starts = [0]
    for size in sizes:
        starts.append(starts[-1] + size)
    return starts


def step_kernel(n, group, layers, per_image, capacity, classes, plan, halves, *refs):
    (
        assign_hbm, label_hbm, turned_hbm, embed_hbm, pos_hbm, class_hbm,
        cin_hbm, cdown_hbm, sin_hbm, sdown_hbm,
    ) = refs[:10]
    refs = refs[10:]
    gin_sum, gdown_sum, rest = refs[:3]
    refs = refs[3:]
    (
        assign_ref, label_ref, turned_ref, embed_ref, pos_ref, class_ref,
        slots_ref, first_u, first_s, qkv, probs, att, second_u, second_s, hidden,
        slope, dqkv, gcur,
        gclass_own, gclass_got, joined, joined_got,
    ) = refs[:22]
    refs = refs[22:]
    patch_ref, column, refs = refs[:halves], refs[halves : 2 * halves], refs[2 * halves :]
    pack, got_slots, refs = refs[:halves], refs[halves : 2 * halves], refs[2 * halves :]
    wbuf, dbuf, refs = refs[: layers + 1], refs[layers + 1 : 2 * layers + 2], refs[2 * layers + 2 :]
    gin, gdown, refs = refs[:layers], refs[layers : 2 * layers], refs[2 * layers :]
    gin_got, gdown_got, refs = refs[:layers], refs[layers : 2 * layers], refs[2 * layers :]
    chains = len(plan)
    packs, refs = refs[:chains], refs[chains:]
    got, held = [], []
    for rows, order in plan:
        count = len(order)
        got.append(refs[:count])
        held.append(refs[count : 2 * count - 1])
        refs = refs[2 * count - 1 :]
    (
        load_sem, own_sem, near_send, near_recv, far_send, far_recv, flat_send, flat_recv,
        w_send, w_recv, g_send, g_recv, c_send, c_recv, r_send, r_recv, j_send, j_recv, o_sem,
    ) = refs
    steps = bits_of(n)
    me = lax.axis_index("client")
    rank = me % group
    shard = me // group
    line = shard // PLANE
    spot = shard % PLANE
    rows_in = sin_hbm.shape[1]
    rows_down = sdown_hbm.shape[1]
    rows, width = gcur.shape
    ff = dbuf[0].shape[0]
    rows_at = layout_of(wbuf[0].shape[1] // n, ff // width, pad_of(width // n))

    loads = [
        pltpu.make_async_copy(source, target, load_sem.at[i])
        for i, (source, target) in enumerate([
            (turned_hbm, turned_ref), (assign_hbm, assign_ref), (label_hbm, label_ref),
            (embed_hbm, embed_ref), (pos_hbm, pos_ref), (class_hbm, class_ref),
            (cin_hbm, wbuf[0]), (cdown_hbm, dbuf[0]),
        ])
    ]
    for c in loads:
        c.start()

    def own_in(layer):
        return pltpu.make_async_copy(
            sin_hbm.at[layer],
            wbuf[layer + 1].at[pl.ds(rank * rows_in, rows_in)],
            own_sem.at[layer, 0],
        )

    def own_down(layer):
        return pltpu.make_async_copy(
            sdown_hbm.at[layer],
            dbuf[layer + 1].at[pl.ds(rank * rows_down, rows_down)],
            own_sem.at[layer, 1],
        )

    def near_peer(i):
        return shard * group + lax.rem(rank + i, group)

    def far_peer(i):
        return (lax.rem(line + i, PLANE) * PLANE + spot) * group + rank

    def flat_peer(i):
        return (line * PLANE + lax.rem(spot + i, PLANE)) * group + rank

    def remote(source, target, send, recv, peer):
        return pltpu.make_async_remote_copy(
            src_ref=source, dst_ref=target, send_sem=send, recv_sem=recv,
            device_id=(peer,), device_id_type=MESH,
        )

    def near(h, i):
        to = lax.rem(rank + i, group)
        return remote(
            patch_ref[h].at[to], column[h].at[line, rank], near_send.at[h, i], near_recv.at[h, i],
            near_peer(i),
        )

    def far(h, i, j):
        if j == 0:
            source, member = patch_ref[h].at[rank], rank
        else:
            member = lax.rem(rank + group - j, group)
            source = column[h].at[line, member]
        return remote(
            source, column[h].at[line, member], far_send.at[h, i, j], far_recv.at[h, i, j],
            far_peer(i),
        )

    def flat(h, i):
        return remote(
            pack[h].at[i], got_slots[h].at[spot], flat_send.at[h, i], flat_recv.at[h, i],
            flat_peer(i),
        )

    def weight_in(layer, i):
        return remote(
            sin_hbm.at[layer],
            wbuf[layer + 1].at[pl.ds(rank * rows_in, rows_in)],
            w_send.at[layer, i, 0], w_recv.at[layer, i, 0], near_peer(i),
        )

    def weight_down(layer, i):
        return remote(
            sdown_hbm.at[layer],
            dbuf[layer + 1].at[pl.ds(rank * rows_down, rows_down)],
            w_send.at[layer, i, 1], w_recv.at[layer, i, 1], near_peer(i),
        )

    def grad_in(layer, i):
        to = lax.rem(rank + i, group)
        return remote(
            gin[layer].at[pl.ds(to * rows_in, rows_in)],
            gin_got[layer].at[i - 1], g_send.at[layer, i, 0], g_recv.at[layer, i, 0], near_peer(i),
        )

    def grad_down(layer, i):
        to = lax.rem(rank + i, group)
        return remote(
            gdown[layer].at[pl.ds(to * rows_down, rows_down)],
            gdown_got[layer].at[i - 1], g_send.at[layer, i, 1], g_recv.at[layer, i, 1],
            near_peer(i),
        )

    def grad_class(i):
        return remote(gclass_own, gclass_got.at[i - 1], c_send.at[i], c_recv.at[i], near_peer(i))

    barrier = pltpu.get_barrier_semaphore()
    peers = [near_peer(i) for i in range(1, group)]
    peers += [far_peer(i) for i in range(1, PLANE)]
    peers += [flat_peer(i) for i in range(1, PLANE)]
    for peer in peers:
        pl.semaphore_signal(barrier, inc=1, device_id=(peer,), device_id_type=MESH)
    for layer in range(layers):
        own_in(layer).start()
        own_down(layer).start()
    loads[0].wait()
    turned = turned_ref[...].astype(F32).T.astype(BF)
    piece = turned.shape[0] // group
    size = piece // halves
    for i in range(group):
        for h in range(halves):
            lo = i * piece + h * size
            patch_ref[h][i] = turned[lo : lo + size]
    pl.semaphore_wait(barrier, len(peers))

    for h in range(halves):
        for i in range(1, group):
            near(h, i).start()
        for i in (2, 1, 3):
            far(h, i, 0).start()
    for layer in range(layers):
        for i in range(1, group):
            weight_in(layer, i).start()
            weight_down(layer, i).start()
    for h in range(halves):
        for j in range(1, group):
            near(h, j).wait_recv()
            for i in (2, 1, 3):
                far(h, i, j).start()
        column[h][line, rank] = patch_ref[h][rank]

    targets = [line * PLANE + lax.rem(spot + i, PLANE) for i in range(PLANE)]
    loads[1].wait()
    loads[2].wait()

    def scan(c, carry):
        there = assign_ref[c]
        out = []
        for i in range(PLANE):
            count, slots = carry[i]
            hit = there == targets[i]
            slots = tuple(
                jnp.where(hit & (count == k), c, slots[k]) for k in range(capacity)
            )
            out.append((count + jnp.where(hit, 1, 0), slots))
        return tuple(out)

    zero = jnp.int32(0)
    table = lax.fori_loop(
        0, n, scan, tuple((zero, tuple(zero for _ in range(capacity))) for _ in range(PLANE))
    )
    filled, slots = table[0]
    images = capacity * per_image
    row = lax.broadcasted_iota(jnp.int32, (images, classes), 0)
    lane = lax.broadcasted_iota(jnp.int32, (images, classes), 1)
    want = jnp.full((images, classes), -1, jnp.int32)
    for k in range(capacity):
        base = slots[k] * (group * per_image) + rank * per_image
        for j in range(per_image):
            lab = jnp.where(k < filled, label_ref[base + j], -1)
            want = jnp.where(row == k * per_image + j, lab, want)
    hot = (lane == want).astype(F32)
    full = (want[:, :1] >= 0).astype(F32)
    loads[5].wait()
    every = class_ref[...].astype(F32)
    chosen = lax.broadcasted_iota(jnp.int32, every.shape, 1) == shard
    cls = jnp.sum(jnp.where(chosen, every, 0.0), axis=1).astype(BF)

    def pick(h, c):
        home = c // group
        return column[h][home // PLANE, c % group]

    for h in range(halves):
        for i in range(1, PLANE):
            for j in range(group):
                far(h, i, j).wait_recv()
        for i in (3, 1, 2):
            for k in range(capacity):
                pack[h][i, k] = pick(h, table[i][1][k])
            flat(h, i).start()
        for k in range(capacity):
            got_slots[h][spot, k] = pick(h, slots[k])
    for c in (3, 4, 6, 7):
        loads[c].wait()
    for h in range(halves):
        for i in range(1, PLANE):
            flat(h, i).wait_recv()
        for k in range(capacity):
            home = slots[k] // group
            lo = k * piece + h * size
            slots_ref[lo : lo + size, :] = got_slots[h][home % PLANE, k]

    x = mm(slots_ref[...], embed_ref[...])
    pos = pos_ref[...].astype(F32)
    gcur[...] = x + jnp.concatenate([pos] * (rows // TOK), axis=0)

    def saved(layer):
        return (
            (first_u.at[layer], first_s.at[layer]), qkv.at[layer], probs.at[layer], att.at[layer],
            (second_u.at[layer], second_s.at[layer]), hidden.at[layer], slope.at[layer],
        )

    for layer in range(layers + 1):
        if layer > 0:
            own_in(layer - 1).wait()
            own_down(layer - 1).wait()
            for i in range(1, group):
                weight_in(layer - 1, i).wait_recv()
                weight_down(layer - 1, i).wait_recv()

        out = block_forward(gcur[...], wbuf[layer], dbuf[layer], *saved(layer))
        gcur[...] = out if layer else out.astype(BF).astype(F32)

    pool = (
        lax.broadcasted_iota(jnp.int32, (images, rows), 1) // TOK
        == lax.broadcasted_iota(jnp.int32, (images, rows), 0)
    ).astype(F32) * (1.0 / TOK)
    unpool = (
        lax.broadcasted_iota(jnp.int32, (rows, images), 0) // TOK
        == lax.broadcasted_iota(jnp.int32, (rows, images), 1)
    ).astype(F32) * (1.0 / TOK)
    u, scale = norm(mm(pool, gcur[...], HIGH))
    pooled = u.astype(BF)
    logits = mm_nt(pooled, cls)
    top = jnp.max(logits, axis=-1, keepdims=True)
    e = jnp.exp(logits - top)
    total = jnp.sum(e, axis=-1, keepdims=True)
    loss = (
        jnp.log(total) + top - jnp.sum(jnp.where(lane == want, logits, 0.0), axis=-1, keepdims=True)
    ) * full
    eye = (
        lax.broadcasted_iota(jnp.int32, (images, images), 0)
        == lax.broadcasted_iota(jnp.int32, (images, images), 1)
    )
    rest[rows_at[-2] : rows_at[-2] + 1, :images] = jnp.sum(
        jnp.where(eye, loss, 0.0), axis=0, keepdims=True
    )
    dlog = ((e / total - hot) * full).astype(BF)
    gclass_own[...] = mm_tn(dlog, pooled).astype(BF)
    for i in range(1, group):
        grad_class(i).start()
    dpool = norm_back(u, scale, mm(dlog, cls))
    gcur[...] = mm(unpool, dpool, HIGH)

    for layer in reversed(range(layers)):
        def put_in(start, lhs, rhs, layer=layer):
            for c in range(0, rhs.shape[1], width):
                gin[layer][:, start + c : start + c + width] = mm_tn(
                    lhs[...], rhs[:, c : c + width]
                ).astype(BF)

        def put_down(h, gb, layer=layer):
            for c in range(0, ff, width):
                gdown[layer][c : c + width] = mm_tn(h[:, c : c + width], gb).astype(BF)

        deep = layer + 1
        gcur[...] = block_backward(
            gcur[...], wbuf[deep], dbuf[deep], *saved(deep), dqkv, put_in, put_down,
        )
        if layer:
            for i in range(1, group):
                grad_down(layer, i).start()
                grad_in(layer, i).start()

    def peer_of(bit):
        return me + (1 << bit) - 2 * (1 << bit) * (me // (1 << bit) % 2)

    def mine(bit):
        return me // (1 << bit) % 2

    def source(c, t):
        return packs[c] if t == 0 else held[c][t - 1]

    def size_at(c, t):
        return packs[c].shape[0] >> (t + 1)

    def copy(c, t):
        bit = plan[c][1][t]
        half = size_at(c, t)
        return remote(
            source(c, t).at[pl.ds((1 - mine(bit)) * half, half)], got[c][t],
            r_send.at[c, t], r_recv.at[c, t], peer_of(bit),
        )

    def join(c):
        bit = steps - 1
        take = plan[UPPER + c][0]
        return remote(
            joined.at[c, 1 - mine(bit), pl.ds(0, take)], joined_got.at[c, pl.ds(0, take)],
            j_send.at[c], j_recv.at[c], peer_of(bit),
        )

    def store_final(c, value):
        if c == LAST or c < UPPER:
            lo = rows_at[-4] if c == LAST else rows_at[1 + c]
            rest[lo : lo + value.shape[0], :] = value
        else:
            side = 1 if c < LOWER else 0
            joined[(c - UPPER) % 2, side, : value.shape[0]] = value.astype(BF)

    progress = [0] * chains

    def advance(c):
        t = progress[c]
        count = len(plan[c][1])
        if t >= count:
            return
        progress[c] = t + 1
        half = size_at(c, t)
        copy(c, t).wait_recv()
        first = mine(plan[c][1][t]) * half
        if t == count - 1:
            store_final(c, source(c, t)[first].astype(F32) + got[c][t][0].astype(F32))
            return

        def add(e, carry):
            held[c][t][e] = (
                source(c, t)[first + e].astype(F32) + got[c][t][e].astype(F32)
            ).astype(BF)
            return carry

        lax.fori_loop(0, half, add, 0)
        copy(c, t + 1).start()

    per_dev = wbuf[0].shape[1] // n
    cols = width // n
    pad = pad_of(cols)
    src = lax.broadcasted_iota(jnp.int32, (width, n * pad), 0)
    dst = lax.broadcasted_iota(jnp.int32, (width, n * pad), 1)
    spread_to = ((dst // pad == src // cols) & (dst % pad == src % cols)).astype(F32).astype(BF)
    tok = (
        lax.broadcasted_iota(jnp.int32, (rows, LANES), 0) % TOK
        == lax.broadcasted_iota(jnp.int32, (rows, LANES), 1)
    ).astype(F32).astype(BF)

    def put_in(start, lhs, rhs):
        base = UPPER if start >= 4 * width else LOWER
        for c in range(0, rhs.shape[1], width):
            part = mm_tn(rhs[:, c : c + width], lhs[...]).astype(BF)
            first = (start + c) // per_dev
            for j in range(width // per_dev):
                lo = j * per_dev
                for piece_at in range(2):
                    take, order = plan[base + piece_at]
                    packs[base + piece_at][place_of(first + j, order)] = part[lo : lo + take]
                    lo += take

    def put_down(h, gb):
        spread = mm(gb, spread_to).astype(BF)
        for q in range(ff // width):
            part = mm_tn(spread, h[:, q * width : (q + 1) * width]).astype(BF)
            c = DOWN + min(q, 2)
            lo = max(q - 2, 0) * pad
            for j in range(n):
                packs[c][place_of(j, plan[c][1]), lo : lo + pad] = part[j * pad : (j + 1) * pad]

    def after(stage):
        if stage == 0:
            for c in range(DOWN, UPPER):
                copy(c, 0).start()
        elif stage == 1:
            for c in range(UPPER, LOWER):
                copy(c, 0).start()
            for c in (DOWN + 2, DOWN, DOWN + 1):
                advance(c)
        elif stage == 3:
            for c in range(UPPER, LOWER):
                advance(c)
        elif stage == 4:
            for c in range(LOWER, LAST):
                copy(c, 0).start()
            for i in range(1, group):
                grad_down(0, i).start()
                grad_in(0, i).start()

    dx = block_backward(
        gcur[...].astype(BF).astype(F32), wbuf[0], dbuf[0], *saved(0), dqkv,
        put_in, put_down, after,
    )
    for c in range(LOWER, LAST):
        advance(c)
    spread = mm(dx.astype(BF), spread_to).astype(BF)
    patch = slots_ref.shape[1]
    embed_part = mm_tn(spread, slots_ref[...]).astype(BF)
    pos_part = mm_tn(spread, tok).astype(BF)
    for j in range(n):
        at = place_of(j, plan[LAST][1])
        packs[LAST][at, :, :patch] = embed_part[j * pad : (j + 1) * pad]
        packs[LAST][at, :, patch : width - LANES] = jnp.zeros((pad, width - LANES - patch), BF)
        packs[LAST][at, :, width - LANES :] = pos_part[j * pad : (j + 1) * pad]
    copy(LAST, 0).start()

    def gin_out(layer):
        return pltpu.make_async_copy(gin_got[layer].at[0], gin_sum.at[layer], o_sem.at[layer, 0])

    def gdown_out(layer):
        return pltpu.make_async_copy(
            gdown_got[layer].at[0], gdown_sum.at[layer], o_sem.at[layer, 1]
        )

    def add_layer(layer):
        for i in range(1, group):
            grad_down(layer, i).wait_recv()
            grad_in(layer, i).wait_recv()
        start = rank * rows_in
        whole = gin[layer][pl.ds(start, rows_in)].astype(F32)
        for i in range(1, group):
            whole = whole + gin_got[layer][i - 1].astype(F32)
        gin_got[layer][0] = whole.astype(BF)
        gin_out(layer).start()
        start = rank * rows_down
        whole = gdown[layer][pl.ds(start, rows_down)].astype(F32)
        for i in range(1, group):
            whole = whole + gdown_got[layer][i - 1].astype(F32)
        gdown_got[layer][0] = whole.astype(BF)
        gdown_out(layer).start()

    def finished(c):
        return progress[c] == len(plan[c][1])

    rounds = 0
    started = [False, False]
    while not all(finished(c) for c in range(chains)):
        for c in (2, 0, 1, UPPER, UPPER + 1, LAST, LOWER, LOWER + 1):
            advance(c)
            for k in range(2):
                if finished(UPPER + k) and finished(LOWER + k) and not started[k]:
                    started[k] = True
                    join(k).start()
        if 0 < rounds <= layers:
            add_layer(layers - rounds)
        rounds += 1
    for i in range(1, group):
        grad_class(i).wait_recv()
    both = gclass_own[...].astype(F32)
    for i in range(1, group):
        both = both + gclass_got[i - 1].astype(F32)
    kept = both[:, :rows_in]
    for i in range(1, group):
        kept = jnp.where(rank == i, both[:, i * rows_in : (i + 1) * rows_in], kept)
    rest[rows_at[-3] : rows_at[-3] + classes, :rows_in] = kept
    lo = 0
    for c in range(2):
        join(c).wait_recv()
        take = plan[UPPER + c][0]
        rest[lo : lo + take, :] = (
            joined[c, mine(steps - 1), :take].astype(F32) + joined_got[c, :take].astype(F32)
        )
        lo += take

    for h in range(halves):
        for i in range(1, group):
            near(h, i).wait_send()
        for i in range(1, PLANE):
            flat(h, i).wait_send()
            for j in range(group):
                far(h, i, j).wait_send()
    for i in range(1, group):
        grad_class(i).wait_send()
        for layer in range(layers):
            weight_in(layer, i).wait_send()
            weight_down(layer, i).wait_send()
            grad_in(layer, i).wait_send()
            grad_down(layer, i).wait_send()
    for c in range(chains):
        for t in range(len(plan[c][1])):
            copy(c, t).wait_send()
    for c in range(2):
        join(c).wait_send()
    for layer in range(layers):
        gin_out(layer).wait()
        gdown_out(layer).wait()


def finish_kernel(
    cuts, rows_at, gin_hbm, gdown_hbm, rest_hbm,
    gin_out, gdown_out, gclass_ref, loss_ref, cin_ref, cdown_ref, embed_ref, pos_ref,
    gin_near, gdown_near, rest, gin_wide, gdown_wide, in_sem, out_sem, rest_sem,
):
    layers, rows_in, rows_down = gin_hbm.shape[0], gin_hbm.shape[1], gdown_hbm.shape[1]
    pieces = []
    for layer in range(layers):
        for j in range(cuts):
            for source, near, wide, out, size, kind in (
                (gin_hbm, gin_near, gin_wide, gin_out, rows_in // cuts, 0),
                (gdown_hbm, gdown_near, gdown_wide, gdown_out, rows_down // cuts, 1),
            ):
                at = (layer, pl.ds(j * size, size))
                pieces.append((
                    pltpu.make_async_copy(source.at[at], near.at[at], in_sem.at[layer, j, kind]),
                    pltpu.make_async_copy(wide.at[at], out.at[at], out_sem.at[layer, j, kind]),
                    near, wide, at,
                ))
    load = pltpu.make_async_copy(rest_hbm, rest, rest_sem)
    load.start()
    for piece in pieces:
        piece[0].start()
    for arrive, leave, near, wide, at in pieces:
        arrive.wait()
        wide[at] = near[at].astype(F32)
        leave.start()
    load.wait()
    cin_ref[...] = rest[: cin_ref.shape[0], :]
    own, width = cdown_ref.shape[0], rest.shape[1]
    for q in range(cdown_ref.shape[1] // width):
        lo = rows_at[1 + q]
        cdown_ref[:, q * width : (q + 1) * width] = rest[lo : lo + own, :]
    last = rest[rows_at[-4] : rows_at[-3], :]
    embed_ref[...] = last[:own, : embed_ref.shape[1]]
    pos_ref[...] = last[:, width - LANES :].T[:TOK, :own]
    classes, shared = gclass_ref.shape
    gclass_ref[...] = rest[rows_at[-3] : rows_at[-3] + classes, :shared]
    loss_ref[...] = rest[rows_at[-2] : rows_at[-2] + 1, : loss_ref.shape[1]]
    for piece in pieces:
        piece[1].wait()


def vmem():
    return pl.BlockSpec(memory_space=pltpu.VMEM)


def hbm():
    return pl.BlockSpec(memory_space=pltpu.HBM)


def shape(dims, kind):
    return jax.ShapeDtypeStruct(dims, kind)


def per_device(
    patches, labels, assign, patch_embed, positions, client_in, client_down,
    server_in, server_down, classifier,
):
    n = lax.axis_size("client")
    group = n // SHARDS
    rows = patches.shape[0]
    patch = patches.shape[1]
    width = client_in.shape[0]
    cols = client_in.shape[1]
    ff = client_down.shape[0]
    layers = server_in.shape[0]
    rows_in = server_in.shape[1]
    rows_down = server_down.shape[1]
    classes = classifier.shape[2]
    piece = rows // group
    halves = 2 if piece % (2 * PAD) == 0 else 1
    per_image = IMG // group
    capacity = SLOTS * group
    s_rows = capacity * piece
    r_in = cols // n
    own = width // n
    steps = bits_of(n)
    pad = pad_of(own)
    plan = chain_plan(n, r_in, ff // width, pad)
    shards = classifier.shape[0]
    rows_at = layout_of(r_in, ff // width, pad)
    per = LANES // (width // HEADS)
    spaces = [
        ((s_rows, width), BF),
        ((s_rows, 1), F32),
        ((s_rows, 3 * width), BF),
        ((s_rows // LANES * (width // LANES), per * LANES, LANES), BF),
        ((s_rows, width), BF),
        ((s_rows, width), BF),
        ((s_rows, 1), F32),
        ((s_rows, ff), BF),
        ((s_rows, ff), BF),
    ]
    scratch = [
        pltpu.SMEM((n,), jnp.int32),
        pltpu.SMEM((n * IMG,), jnp.int32),
        pltpu.VMEM((patch, rows), BF),
        pltpu.VMEM((patch, width), BF),
        pltpu.VMEM((TOK, width), BF),
        pltpu.VMEM((classes, shards, width), BF),
        pltpu.VMEM((s_rows, patch), BF),
    ]
    scratch += [pltpu.VMEM((layers + 1,) + dims, kind) for dims, kind in spaces]
    scratch += [
        pltpu.VMEM((s_rows, 3 * width), BF),
        pltpu.VMEM((s_rows, width), F32),
        pltpu.VMEM((classes, width), BF),
        pltpu.VMEM((group - 1, classes, width), BF),
        pltpu.VMEM((2, 2, plan[UPPER][0], width), BF),
        pltpu.VMEM((2, plan[UPPER][0], width), BF),
    ]
    for dims in ((group,), (PLANE, group), (PLANE, capacity), (PLANE, capacity)):
        scratch += [pltpu.VMEM(dims + (piece // halves, patch), BF)] * halves
    scratch += [pltpu.VMEM((width, cols), BF)] * (layers + 1)
    scratch += [pltpu.VMEM((ff, width), BF)] * (layers + 1)
    scratch += [pltpu.VMEM((width, cols), BF)] * layers
    scratch += [pltpu.VMEM((ff, width), BF)] * layers
    scratch += [pltpu.VMEM((group - 1, rows_in, cols), BF)] * layers
    scratch += [pltpu.VMEM((group - 1, rows_down, width), BF)] * layers
    scratch += [pltpu.VMEM((1 << len(order), r, width), BF) for r, order in plan]
    for r, order in plan:
        count = len(order)
        scratch += [pltpu.VMEM((1 << (count - 1 - t), r, width), BF) for t in range(count)]
        scratch += [pltpu.VMEM((1 << (count - 1 - t), r, width), BF) for t in range(count - 1)]
    scratch += [
        pltpu.SemaphoreType.DMA(dims)
        for dims in [
            (8,), (layers, 2), (halves, group), (halves, group), (halves, PLANE, group),
            (halves, PLANE, group), (halves, PLANE), (halves, PLANE), (layers, group, 2), (layers, group, 2), (layers, group, 2),
            (layers, group, 2), (group,), (group,), (len(plan), steps), (len(plan), steps),
            (2,), (2,), (layers, 2),
        ]
    ]
    found = pl.pallas_call(
        functools.partial(
            step_kernel, n, group, layers, per_image, capacity, classes, plan, halves
        ),
        out_shape=[
            shape((layers, rows_in, cols), BF),
            shape((layers, rows_down, width), BF),
            shape((rows_at[-1], width), F32),
        ],
        in_specs=[hbm()] * 10,
        out_specs=[hbm(), hbm(), vmem()],
        scratch_shapes=scratch,
        compiler_params=pltpu.CompilerParams(
            collective_id=1, has_side_effects=True, vmem_limit_bytes=VMEM_LIMIT
        ),
    )(
        assign.reshape(n), labels, patches.T, patch_embed, positions,
        classifier.transpose(2, 0, 1), client_in, client_down, server_in, server_down,
    )
    cuts = 4 if rows_in % (4 * PAD) == 0 else 1
    gin, gdown, gclass, loss, cin, cdown, embed, pos = pl.pallas_call(
        functools.partial(finish_kernel, cuts, rows_at),
        out_shape=[
            shape((layers, rows_in, cols), F32),
            shape((layers, rows_down, width), F32),
            shape((classes, rows_in), F32),
            shape((1, capacity * per_image), F32),
            shape((r_in, width), F32),
            shape((own, ff), F32),
            shape((own, patch), F32),
            shape((TOK, own), F32),
        ],
        in_specs=[hbm()] * 3,
        out_specs=[hbm()] * 2 + [vmem()] * 6,
        scratch_shapes=[
            pltpu.VMEM((layers, rows_in, cols), BF),
            pltpu.VMEM((layers, rows_down, width), BF),
            pltpu.VMEM((rows_at[-1], width), F32),
            pltpu.VMEM((layers, rows_in, cols), F32),
            pltpu.VMEM((layers, rows_down, width), F32),
            pltpu.SemaphoreType.DMA((layers, cuts, 2)),
            pltpu.SemaphoreType.DMA((layers, cuts, 2)),
            pltpu.SemaphoreType.DMA,
        ],
        compiler_params=pltpu.CompilerParams(vmem_limit_bytes=24 * 1024 * 1024),
    )(*found)
    return loss, embed.T, pos, cin.T, cdown.T, gin, gdown, gclass.T


def solution(mesh):
    whole = P()
    in_specs = (
        P("client", None), whole, whole, whole, whole, whole, whole,
        P(None, "client", None), P(None, "client", None), whole,
    )
    out_specs = (
        P("client", None), P(None, "client"), P(None, "client"), P(None, "client"),
        P(None, "client"), P(None, "client", None), P(None, "client", None), P("client", None),
    )
    return jax.shard_map(
        per_device, mesh=mesh, in_specs=in_specs, out_specs=out_specs, check_vma=False
    )
```

```python
import functools
import math

import jax
import jax.numpy as jnp
from jax import lax
from jax.experimental import pallas as pl
from jax.experimental.pallas import tpu as pltpu
from jax.sharding import PartitionSpec as P

HEADS = 6
TOK = 16
IMG = 8
SHARDS = 16
SLOTS = 2
PLANE = 4
EPSILON = 1e-06
LANES = 128
PAD = 16
BF = jnp.bfloat16
F32 = jnp.float32
HIGH = lax.Precision.HIGHEST
GELU_C = math.sqrt(2.0 / math.pi)
VMEM_LIMIT = 60 * 1024 * 1024
MESH = pl.DeviceIdType.MESH


def mm(a, b, precision=None):
    return lax.dot_general(
        a, b, (((1,), (0,)), ((), ())), precision=precision, preferred_element_type=F32
    )


def mm_nt(a, b, precision=None):
    return lax.dot_general(
        a, b, (((1,), (1,)), ((), ())), precision=precision, preferred_element_type=F32
    )


def mm_tn(a, b):
    return lax.dot_general(a, b, (((0,), (0,)), ((), ())), preferred_element_type=F32)


def norm(v):
    centre = v - jnp.mean(v, axis=-1, keepdims=True)
    scale = lax.rsqrt(jnp.mean(centre * centre, axis=-1, keepdims=True) + EPSILON)
    return centre * scale, scale


def norm_back(normed, scale, grad):
    return scale * (
        grad
        - jnp.mean(grad, axis=-1, keepdims=True)
        - normed * jnp.mean(grad * normed, axis=-1, keepdims=True)
    )


def gelu_both(v):
    sq = v * v
    t = jnp.tanh(v * (GELU_C + (GELU_C * 0.044715) * sq))
    half = 0.5 + 0.5 * t
    slope = half + (0.5 * v) * (1.0 - t * t) * (GELU_C + (GELU_C * 0.134145) * sq)
    return v * half, slope


def image_mask(per):
    row = lax.broadcasted_iota(jnp.int32, (per * LANES, LANES), 0) % LANES
    col = lax.broadcasted_iota(jnp.int32, (per * LANES, LANES), 1)
    return row // TOK == col // TOK


def lane_masks(head_dim):
    lane = lax.broadcasted_iota(jnp.int32, (LANES, LANES), 1)
    return [lane // head_dim == h for h in range(LANES // head_dim)]


def stack(value, keeps):
    return jnp.concatenate([jnp.where(k, value, jnp.zeros_like(value)) for k in keeps], axis=0)


def widen(value, per):
    return jnp.concatenate(
        [value[h * LANES : (h + 1) * LANES] for h in range(per)], axis=1
    )


def attend(qkv_ref, probs_ref, att_ref, width):
    rows = qkv_ref.shape[0]
    head_dim = width // HEADS
    per = LANES // head_dim
    inside = image_mask(per)
    keeps = lane_masks(head_dim)
    for group in range(rows // LANES):
        r = slice(group * LANES, (group + 1) * LANES)
        for pair in range(width // LANES):
            lo = pair * LANES
            q = qkv_ref[r, lo : lo + LANES]
            k = qkv_ref[r, width + lo : width + lo + LANES]
            v = qkv_ref[r, 2 * width + lo : 2 * width + lo + LANES]
            s = jnp.where(inside, mm_nt(stack(q, keeps), k), -1e30)
            e = jnp.exp(s - jnp.max(s, axis=-1, keepdims=True))
            p = (e * (1.0 / jnp.sum(e, axis=-1, keepdims=True))).astype(BF)
            probs_ref[group * (width // LANES) + pair] = p
            att_ref[r, lo : lo + LANES] = mm(widen(p, per), stack(v, keeps)).astype(BF)


def attend_back(grad, qkv_ref, probs_ref, dqkv_ref, width):
    rows = qkv_ref.shape[0]
    head_dim = width // HEADS
    per = LANES // head_dim
    keeps = lane_masks(head_dim)
    for group in range(rows // LANES):
        r = slice(group * LANES, (group + 1) * LANES)
        for pair in range(width // LANES):
            lo = pair * LANES
            q = qkv_ref[r, lo : lo + LANES]
            k = qkv_ref[r, width + lo : width + lo + LANES]
            v = qkv_ref[r, 2 * width + lo : 2 * width + lo + LANES]
            go = stack(grad[r, lo : lo + LANES].astype(BF), keeps)
            p = probs_ref[group * (width // LANES) + pair]
            dp = mm_nt(go, v)
            dv = mm_tn(p, go)
            pf = p.astype(F32)
            ds = (pf * (dp - jnp.sum(pf * dp, axis=-1, keepdims=True))).astype(BF)
            dq = mm(widen(ds, per), stack(k, keeps)) * (1.0 / math.sqrt(head_dim))
            dk = mm_tn(ds, stack(q, keeps))
            dqkv_ref[r, lo : lo + LANES] = dq.astype(BF)
            dqkv_ref[r, width + lo : width + lo + LANES] = dk.astype(BF)
            dqkv_ref[r, 2 * width + lo : 2 * width + lo + LANES] = dv.astype(BF)


def block_forward(x, w_ref, d_ref, first, qkv_ref, probs_ref, att_ref, second, h_ref, slope_ref):
    width = x.shape[1]
    ff = d_ref.shape[0]
    u, scale = norm(x)
    u = u.astype(BF)
    first[0][...] = u
    first[1][...] = scale
    for part in range(3):
        value = mm(u, w_ref[:, part * width : (part + 1) * width])
        if part == 0:
            value = value * (1.0 / math.sqrt(width // HEADS))
        qkv_ref[:, part * width : (part + 1) * width] = value.astype(BF)
    attend(qkv_ref, probs_ref, att_ref, width)
    y = x + mm(att_ref[...], w_ref[:, 3 * width : 4 * width])
    u, scale = norm(y)
    u = u.astype(BF)
    second[0][...] = u
    second[1][...] = scale
    for lo in range(0, ff, width):
        value, slope = gelu_both(mm(u, w_ref[:, 4 * width + lo : 5 * width + lo]))
        h_ref[:, lo : lo + width] = value.astype(BF)
        slope_ref[:, lo : lo + width] = slope.astype(BF)
    return y + mm(h_ref[...], d_ref[...])


def block_backward(
    g, w_ref, d_ref, first, qkv_ref, probs_ref, att_ref, second, h_ref, slope_ref, dqkv_ref,
    put_in, put_down, after=lambda stage: None,
):
    width = g.shape[1]
    ff = d_ref.shape[0]
    gb = g.astype(BF)
    put_down(h_ref, gb)
    after(0)
    for lo in range(0, ff, width):
        slope = slope_ref[:, lo : lo + width].astype(F32)
        slope_ref[:, lo : lo + width] = (mm_nt(gb, d_ref[lo : lo + width, :]) * slope).astype(BF)
    put_in(4 * width, second[0], slope_ref)
    after(1)
    dy = g + norm_back(
        second[0][...].astype(F32), second[1][...], mm_nt(slope_ref[...], w_ref[:, 4 * width :])
    )
    gb = dy.astype(BF)
    dqkv_ref[:, :width] = gb
    put_in(3 * width, att_ref, dqkv_ref.at[:, :width])
    after(2)
    attend_back(
        mm_nt(gb, w_ref[:, 3 * width : 4 * width]), qkv_ref, probs_ref, dqkv_ref, width
    )
    after(3)
    put_in(0, first[0], dqkv_ref)
    after(4)
    return dy + norm_back(
        first[0][...].astype(F32), first[1][...], mm_nt(dqkv_ref[...], w_ref[:, : 3 * width])
    )


def bits_of(n):
    return n.bit_length() - 1


def place_of(device, order):
    index = 0
    for bit in order:
        index = index * 2 + (device >> bit & 1)
    return index


def pad_of(own):
    return (own + 7) // 8 * 8


def chain_plan(n, r_in, blocks, pad):
    steps = bits_of(n)
    rest = list(range(1, steps))
    far = rest[-2:]
    near = rest[:-2]
    low = near[: len(near) // 2]
    high = near[len(near) // 2 :]
    first = [0] + low + high + far
    second = [0] + high + low + far
    third = [0] + far + low + high
    top = (r_in // 2 + PAD - 1) // PAD * PAD
    return [
        (pad, first), (pad, second), ((blocks - 2) * pad, third),
        (top, first[:-1]), (r_in - top, second[:-1]),
        (top, first[:-1]), (r_in - top, second[:-1]),
        (pad, third),
    ]


DOWN, UPPER, LOWER, LAST = 0, 3, 5, 7


def layout_of(r_in, blocks, pad):
    sizes = [r_in] + [pad] * (blocks + 1) + [16, 8]
    starts = [0]
    for size in sizes:
        starts.append(starts[-1] + size)
    return starts


def step_kernel(n, group, layers, per_image, capacity, classes, plan, halves, *refs):
    (
        assign_hbm, label_hbm, turned_hbm, embed_hbm, pos_hbm, class_hbm,
        cin_hbm, cdown_hbm, sin_hbm, sdown_hbm,
    ) = refs[:10]
    refs = refs[10:]
    gin_sum, gdown_sum, rest = refs[:3]
    refs = refs[3:]
    (
        assign_ref, label_ref, turned_ref, embed_ref, pos_ref, class_ref,
        slots_ref, first_u, first_s, qkv, probs, att, second_u, second_s, hidden,
        slope, dqkv, gcur,
        gclass_own, gclass_got, joined, joined_got,
    ) = refs[:22]
    refs = refs[22:]
    patch_ref, column, refs = refs[:halves], refs[halves : 2 * halves], refs[2 * halves :]
    pack, got_slots, refs = refs[:halves], refs[halves : 2 * halves], refs[2 * halves :]
    wbuf, dbuf, refs = refs[: layers + 1], refs[layers + 1 : 2 * layers + 2], refs[2 * layers + 2 :]
    gin, gdown, refs = refs[:layers], refs[layers : 2 * layers], refs[2 * layers :]
    gin_got, gdown_got, refs = refs[:layers], refs[layers : 2 * layers], refs[2 * layers :]
    chains = len(plan)
    packs, refs = refs[:chains], refs[chains:]
    got, held = [], []
    for rows, order in plan:
        count = len(order)
        got.append(refs[:count])
        held.append(refs[count : 2 * count - 1])
        refs = refs[2 * count - 1 :]
    (
        load_sem, own_sem, near_send, near_recv, far_send, far_recv, flat_send, flat_recv,
        w_send, w_recv, g_send, g_recv, c_send, c_recv, r_send, r_recv, j_send, j_recv, o_sem,
    ) = refs
    steps = bits_of(n)
    me = lax.axis_index("client")
    rank = me % group
    shard = me // group
    line = shard // PLANE
    spot = shard % PLANE
    rows_in = sin_hbm.shape[1]
    rows_down = sdown_hbm.shape[1]
    rows, width = gcur.shape
    ff = dbuf[0].shape[0]
    rows_at = layout_of(wbuf[0].shape[1] // n, ff // width, pad_of(width // n))

    loads = [
        pltpu.make_async_copy(source, target, load_sem.at[i])
        for i, (source, target) in enumerate([
            (turned_hbm, turned_ref), (assign_hbm, assign_ref), (label_hbm, label_ref),
            (embed_hbm, embed_ref), (pos_hbm, pos_ref), (class_hbm, class_ref),
            (cin_hbm, wbuf[0]), (cdown_hbm, dbuf[0]),
        ])
    ]
    for c in loads:
        c.start()

    def own_in(layer):
        return pltpu.make_async_copy(
            sin_hbm.at[layer],
            wbuf[layer + 1].at[pl.ds(rank * rows_in, rows_in)],
            own_sem.at[layer, 0],
        )

    def own_down(layer):
        return pltpu.make_async_copy(
            sdown_hbm.at[layer],
            dbuf[layer + 1].at[pl.ds(rank * rows_down, rows_down)],
            own_sem.at[layer, 1],
        )

    def near_peer(i):
        return shard * group + lax.rem(rank + i, group)

    def far_peer(i):
        return (lax.rem(line + i, PLANE) * PLANE + spot) * group + rank

    def flat_peer(i):
        return (line * PLANE + lax.rem(spot + i, PLANE)) * group + rank

    def remote(source, target, send, recv, peer):
        return pltpu.make_async_remote_copy(
            src_ref=source, dst_ref=target, send_sem=send, recv_sem=recv,
            device_id=(peer,), device_id_type=MESH,
        )

    def near(h, i):
        to = lax.rem(rank + i, group)
        return remote(
            patch_ref[h].at[to], column[h].at[line, rank], near_send.at[h, i], near_recv.at[h, i],
            near_peer(i),
        )

    def far(h, i, j):
        if j == 0:
            source, member = patch_ref[h].at[rank], rank
        else:
            member = lax.rem(rank + group - j, group)
            source = column[h].at[line, member]
        return remote(
            source, column[h].at[line, member], far_send.at[h, i, j], far_recv.at[h, i, j],
            far_peer(i),
        )

    def flat(h, i):
        return remote(
            pack[h].at[i], got_slots[h].at[spot], flat_send.at[h, i], flat_recv.at[h, i],
            flat_peer(i),
        )

    def weight_in(layer, i):
        return remote(
            sin_hbm.at[layer],
            wbuf[layer + 1].at[pl.ds(rank * rows_in, rows_in)],
            w_send.at[layer, i, 0], w_recv.at[layer, i, 0], near_peer(i),
        )

    def weight_down(layer, i):
        return remote(
            sdown_hbm.at[layer],
            dbuf[layer + 1].at[pl.ds(rank * rows_down, rows_down)],
            w_send.at[layer, i, 1], w_recv.at[layer, i, 1], near_peer(i),
        )

    def grad_in(layer, i):
        to = lax.rem(rank + i, group)
        return remote(
            gin[layer].at[pl.ds(to * rows_in, rows_in)],
            gin_got[layer].at[i - 1], g_send.at[layer, i, 0], g_recv.at[layer, i, 0], near_peer(i),
        )

    def grad_down(layer, i):
        to = lax.rem(rank + i, group)
        return remote(
            gdown[layer].at[pl.ds(to * rows_down, rows_down)],
            gdown_got[layer].at[i - 1], g_send.at[layer, i, 1], g_recv.at[layer, i, 1],
            near_peer(i),
        )

    def grad_class(i):
        return remote(gclass_own, gclass_got.at[i - 1], c_send.at[i], c_recv.at[i], near_peer(i))

    barrier = pltpu.get_barrier_semaphore()
    peers = [near_peer(i) for i in range(1, group)]
    peers += [far_peer(i) for i in range(1, PLANE)]
    peers += [flat_peer(i) for i in range(1, PLANE)]
    for peer in peers:
        pl.semaphore_signal(barrier, inc=1, device_id=(peer,), device_id_type=MESH)
    for layer in range(layers):
        own_in(layer).start()
        own_down(layer).start()
    loads[0].wait()
    turned = turned_ref[...].astype(F32).T.astype(BF)
    piece = turned.shape[0] // group
    size = piece // halves
    for i in range(group):
        for h in range(halves):
            lo = i * piece + h * size
            patch_ref[h][i] = turned[lo : lo + size]
    pl.semaphore_wait(barrier, len(peers))

    for h in range(halves):
        for i in range(1, group):
            near(h, i).start()
        for i in (2, 1, 3):
            far(h, i, 0).start()
    for layer in range(layers):
        for i in range(1, group):
            weight_in(layer, i).start()
            weight_down(layer, i).start()
    for h in range(halves):
        for j in range(1, group):
            near(h, j).wait_recv()
            for i in (2, 1, 3):
                far(h, i, j).start()
        column[h][line, rank] = patch_ref[h][rank]

    targets = [line * PLANE + lax.rem(spot + i, PLANE) for i in range(PLANE)]
    loads[1].wait()
    loads[2].wait()

    def scan(c, carry):
        there = assign_ref[c]
        out = []
        for i in range(PLANE):
            count, slots = carry[i]
            hit = there == targets[i]
            slots = tuple(
                jnp.where(hit & (count == k), c, slots[k]) for k in range(capacity)
            )
            out.append((count + jnp.where(hit, 1, 0), slots))
        return tuple(out)

    zero = jnp.int32(0)
    table = lax.fori_loop(
        0, n, scan, tuple((zero, tuple(zero for _ in range(capacity))) for _ in range(PLANE))
    )
    filled, slots = table[0]
    images = capacity * per_image
    row = lax.broadcasted_iota(jnp.int32, (images, classes), 0)
    lane = lax.broadcasted_iota(jnp.int32, (images, classes), 1)
    want = jnp.full((images, classes), -1, jnp.int32)
    for k in range(capacity):
        base = slots[k] * (group * per_image) + rank * per_image
        for j in range(per_image):
            lab = jnp.where(k < filled, label_ref[base + j], -1)
            want = jnp.where(row == k * per_image + j, lab, want)
    hot = (lane == want).astype(F32)
    full = (want[:, :1] >= 0).astype(F32)
    loads[5].wait()
    every = class_ref[...].astype(F32)
    chosen = lax.broadcasted_iota(jnp.int32, every.shape, 1) == shard
    cls = jnp.sum(jnp.where(chosen, every, 0.0), axis=1).astype(BF)

    def pick(h, c):
        home = c // group
        return column[h][home // PLANE, c % group]

    for h in range(halves):
        for i in range(1, PLANE):
            for j in range(group):
                far(h, i, j).wait_recv()
        for i in (3, 1, 2):
            for k in range(capacity):
                pack[h][i, k] = pick(h, table[i][1][k])
            flat(h, i).start()
        for k in range(capacity):
            got_slots[h][spot, k] = pick(h, slots[k])
    for c in (3, 4, 6, 7):
        loads[c].wait()
    for h in range(halves):
        for i in range(1, PLANE):
            flat(h, i).wait_recv()
        for k in range(capacity):
            home = slots[k] // group
            lo = k * piece + h * size
            slots_ref[lo : lo + size, :] = got_slots[h][home % PLANE, k]

    x = mm(slots_ref[...], embed_ref[...])
    pos = pos_ref[...].astype(F32)
    gcur[...] = x + jnp.concatenate([pos] * (rows // TOK), axis=0)

    def saved(layer):
        return (
            (first_u.at[layer], first_s.at[layer]), qkv.at[layer], probs.at[layer], att.at[layer],
            (second_u.at[layer], second_s.at[layer]), hidden.at[layer], slope.at[layer],
        )

    for layer in range(layers + 1):
        if layer > 0:
            own_in(layer - 1).wait()
            own_down(layer - 1).wait()
            for i in range(1, group):
                weight_in(layer - 1, i).wait_recv()
                weight_down(layer - 1, i).wait_recv()

        out = block_forward(gcur[...], wbuf[layer], dbuf[layer], *saved(layer))
        gcur[...] = out if layer else out.astype(BF).astype(F32)

    pool = (
        lax.broadcasted_iota(jnp.int32, (images, rows), 1) // TOK
        == lax.broadcasted_iota(jnp.int32, (images, rows), 0)
    ).astype(F32) * (1.0 / TOK)
    unpool = (
        lax.broadcasted_iota(jnp.int32, (rows, images), 0) // TOK
        == lax.broadcasted_iota(jnp.int32, (rows, images), 1)
    ).astype(F32) * (1.0 / TOK)
    u, scale = norm(mm(pool, gcur[...], HIGH))
    pooled = u.astype(BF)
    logits = mm_nt(pooled, cls)
    top = jnp.max(logits, axis=-1, keepdims=True)
    e = jnp.exp(logits - top)
    total = jnp.sum(e, axis=-1, keepdims=True)
    loss = (
        jnp.log(total) + top - jnp.sum(jnp.where(lane == want, logits, 0.0), axis=-1, keepdims=True)
    ) * full
    eye = (
        lax.broadcasted_iota(jnp.int32, (images, images), 0)
        == lax.broadcasted_iota(jnp.int32, (images, images), 1)
    )
    rest[rows_at[-2] : rows_at[-2] + 1, :images] = jnp.sum(
        jnp.where(eye, loss, 0.0), axis=0, keepdims=True
    )
    dlog = ((e / total - hot) * full).astype(BF)
    gclass_own[...] = mm_tn(dlog, pooled).astype(BF)
    for i in range(1, group):
        grad_class(i).start()
    dpool = norm_back(u, scale, mm(dlog, cls))
    gcur[...] = mm(unpool, dpool, HIGH)

    for layer in reversed(range(layers)):
        def put_in(start, lhs, rhs, layer=layer):
            for c in range(0, rhs.shape[1], width):
                gin[layer][:, start + c : start + c + width] = mm_tn(
                    lhs[...], rhs[:, c : c + width]
                ).astype(BF)

        def put_down(h, gb, layer=layer):
            for c in range(0, ff, width):
                gdown[layer][c : c + width] = mm_tn(h[:, c : c + width], gb).astype(BF)

        deep = layer + 1
        gcur[...] = block_backward(
            gcur[...], wbuf[deep], dbuf[deep], *saved(deep), dqkv, put_in, put_down,
        )
        if layer:
            for i in range(1, group):
                grad_down(layer, i).start()
                grad_in(layer, i).start()

    def peer_of(bit):
        return me + (1 << bit) - 2 * (1 << bit) * (me // (1 << bit) % 2)

    def mine(bit):
        return me // (1 << bit) % 2

    def source(c, t):
        return packs[c] if t == 0 else held[c][t - 1]

    def size_at(c, t):
        return packs[c].shape[0] >> (t + 1)

    def copy(c, t):
        bit = plan[c][1][t]
        half = size_at(c, t)
        return remote(
            source(c, t).at[pl.ds((1 - mine(bit)) * half, half)], got[c][t],
            r_send.at[c, t], r_recv.at[c, t], peer_of(bit),
        )

    def join(c):
        bit = steps - 1
        take = plan[UPPER + c][0]
        return remote(
            joined.at[c, 1 - mine(bit), pl.ds(0, take)], joined_got.at[c, pl.ds(0, take)],
            j_send.at[c], j_recv.at[c], peer_of(bit),
        )

    def store_final(c, value):
        if c == LAST or c < UPPER:
            lo = rows_at[-4] if c == LAST else rows_at[1 + c]
            rest[lo : lo + value.shape[0], :] = value
        else:
            side = 1 if c < LOWER else 0
            joined[(c - UPPER) % 2, side, : value.shape[0]] = value.astype(BF)

    progress = [0] * chains

    def advance(c):
        t = progress[c]
        count = len(plan[c][1])
        if t >= count:
            return
        progress[c] = t + 1
        half = size_at(c, t)
        copy(c, t).wait_recv()
        first = mine(plan[c][1][t]) * half
        if t == count - 1:
            store_final(c, source(c, t)[first].astype(F32) + got[c][t][0].astype(F32))
            return

        def add(e, carry):
            held[c][t][e] = (
                source(c, t)[first + e].astype(F32) + got[c][t][e].astype(F32)
            ).astype(BF)
            return carry

        lax.fori_loop(0, half, add, 0)
        copy(c, t + 1).start()

    per_dev = wbuf[0].shape[1] // n
    cols = width // n
    pad = pad_of(cols)
    src = lax.broadcasted_iota(jnp.int32, (width, n * pad), 0)
    dst = lax.broadcasted_iota(jnp.int32, (width, n * pad), 1)
    spread_to = ((dst // pad == src // cols) & (dst % pad == src % cols)).astype(F32).astype(BF)
    tok = (
        lax.broadcasted_iota(jnp.int32, (rows, LANES), 0) % TOK
        == lax.broadcasted_iota(jnp.int32, (rows, LANES), 1)
    ).astype(F32).astype(BF)

    def put_in(start, lhs, rhs):
        base = UPPER if start >= 4 * width else LOWER
        for c in range(0, rhs.shape[1], width):
            part = mm_tn(rhs[:, c : c + width], lhs[...]).astype(BF)
            first = (start + c) // per_dev
            for j in range(width // per_dev):
                lo = j * per_dev
                for piece_at in range(2):
                    take, order = plan[base + piece_at]
                    packs[base + piece_at][place_of(first + j, order)] = part[lo : lo + take]
                    lo += take

    def put_down(h, gb):
        spread = mm(gb, spread_to).astype(BF)
        for q in range(ff // width):
            part = mm_tn(spread, h[:, q * width : (q + 1) * width]).astype(BF)
            c = DOWN + min(q, 2)
            lo = max(q - 2, 0) * pad
            for j in range(n):
                packs[c][place_of(j, plan[c][1]), lo : lo + pad] = part[j * pad : (j + 1) * pad]

    def after(stage):
        if stage == 0:
            for c in range(DOWN, UPPER):
                copy(c, 0).start()
        elif stage == 1:
            for c in range(UPPER, LOWER):
                copy(c, 0).start()
        elif stage == 2:
            for c in (DOWN + 2, DOWN, DOWN + 1):
                advance(c)
        elif stage == 3:
            for c in range(UPPER, LOWER):
                advance(c)
        elif stage == 4:
            for c in range(LOWER, LAST):
                copy(c, 0).start()
            for i in range(1, group):
                grad_down(0, i).start()
                grad_in(0, i).start()

    dx = block_backward(
        gcur[...].astype(BF).astype(F32), wbuf[0], dbuf[0], *saved(0), dqkv,
        put_in, put_down, after,
    )
    for c in range(LOWER, LAST):
        advance(c)
    spread = mm(dx.astype(BF), spread_to).astype(BF)
    patch = slots_ref.shape[1]
    embed_part = mm_tn(spread, slots_ref[...]).astype(BF)
    pos_part = mm_tn(spread, tok).astype(BF)
    for j in range(n):
        at = place_of(j, plan[LAST][1])
        packs[LAST][at, :, :patch] = embed_part[j * pad : (j + 1) * pad]
        packs[LAST][at, :, patch : width - LANES] = jnp.zeros((pad, width - LANES - patch), BF)
        packs[LAST][at, :, width - LANES :] = pos_part[j * pad : (j + 1) * pad]
    copy(LAST, 0).start()

    def gin_out(layer):
        return pltpu.make_async_copy(gin_got[layer].at[0], gin_sum.at[layer], o_sem.at[layer, 0])

    def gdown_out(layer):
        return pltpu.make_async_copy(
            gdown_got[layer].at[0], gdown_sum.at[layer], o_sem.at[layer, 1]
        )

    def add_layer(layer):
        for i in range(1, group):
            grad_down(layer, i).wait_recv()
            grad_in(layer, i).wait_recv()
        start = rank * rows_in
        whole = gin[layer][pl.ds(start, rows_in)].astype(F32)
        for i in range(1, group):
            whole = whole + gin_got[layer][i - 1].astype(F32)
        gin_got[layer][0] = whole.astype(BF)
        gin_out(layer).start()
        start = rank * rows_down
        whole = gdown[layer][pl.ds(start, rows_down)].astype(F32)
        for i in range(1, group):
            whole = whole + gdown_got[layer][i - 1].astype(F32)
        gdown_got[layer][0] = whole.astype(BF)
        gdown_out(layer).start()

    def finished(c):
        return progress[c] == len(plan[c][1])

    rounds = 0
    started = [False, False]
    while not all(finished(c) for c in range(chains)):
        for c in (2, 0, 1, UPPER, UPPER + 1, LAST, LOWER, LOWER + 1):
            advance(c)
            for k in range(2):
                if finished(UPPER + k) and finished(LOWER + k) and not started[k]:
                    started[k] = True
                    join(k).start()
        if 0 < rounds <= layers:
            add_layer(layers - rounds)
        rounds += 1
    for i in range(1, group):
        grad_class(i).wait_recv()
    both = gclass_own[...].astype(F32)
    for i in range(1, group):
        both = both + gclass_got[i - 1].astype(F32)
    kept = both[:, :rows_in]
    for i in range(1, group):
        kept = jnp.where(rank == i, both[:, i * rows_in : (i + 1) * rows_in], kept)
    rest[rows_at[-3] : rows_at[-3] + classes, :rows_in] = kept
    lo = 0
    for c in range(2):
        join(c).wait_recv()
        take = plan[UPPER + c][0]
        rest[lo : lo + take, :] = (
            joined[c, mine(steps - 1), :take].astype(F32) + joined_got[c, :take].astype(F32)
        )
        lo += take

    for h in range(halves):
        for i in range(1, group):
            near(h, i).wait_send()
        for i in range(1, PLANE):
            flat(h, i).wait_send()
            for j in range(group):
                far(h, i, j).wait_send()
    for i in range(1, group):
        grad_class(i).wait_send()
        for layer in range(layers):
            weight_in(layer, i).wait_send()
            weight_down(layer, i).wait_send()
            grad_in(layer, i).wait_send()
            grad_down(layer, i).wait_send()
    for c in range(chains):
        for t in range(len(plan[c][1])):
            copy(c, t).wait_send()
    for c in range(2):
        join(c).wait_send()
    for layer in range(layers):
        gin_out(layer).wait()
        gdown_out(layer).wait()


def finish_kernel(
    cuts, rows_at, gin_hbm, gdown_hbm, rest_hbm,
    gin_out, gdown_out, gclass_ref, loss_ref, cin_ref, cdown_ref, embed_ref, pos_ref,
    gin_near, gdown_near, rest, gin_wide, gdown_wide, in_sem, out_sem, rest_sem,
):
    layers, rows_in, rows_down = gin_hbm.shape[0], gin_hbm.shape[1], gdown_hbm.shape[1]
    pieces = []
    for layer in range(layers):
        for j in range(cuts):
            for source, near, wide, out, size, kind in (
                (gin_hbm, gin_near, gin_wide, gin_out, rows_in // cuts, 0),
                (gdown_hbm, gdown_near, gdown_wide, gdown_out, rows_down // cuts, 1),
            ):
                at = (layer, pl.ds(j * size, size))
                pieces.append((
                    pltpu.make_async_copy(source.at[at], near.at[at], in_sem.at[layer, j, kind]),
                    pltpu.make_async_copy(wide.at[at], out.at[at], out_sem.at[layer, j, kind]),
                    near, wide, at,
                ))
    load = pltpu.make_async_copy(rest_hbm, rest, rest_sem)
    load.start()
    for piece in pieces:
        piece[0].start()
    for arrive, leave, near, wide, at in pieces:
        arrive.wait()
        wide[at] = near[at].astype(F32)
        leave.start()
    load.wait()
    cin_ref[...] = rest[: cin_ref.shape[0], :]
    own, width = cdown_ref.shape[0], rest.shape[1]
    for q in range(cdown_ref.shape[1] // width):
        lo = rows_at[1 + q]
        cdown_ref[:, q * width : (q + 1) * width] = rest[lo : lo + own, :]
    last = rest[rows_at[-4] : rows_at[-3], :]
    embed_ref[...] = last[:own, : embed_ref.shape[1]]
    pos_ref[...] = last[:, width - LANES :].T[:TOK, :own]
    classes, shared = gclass_ref.shape
    gclass_ref[...] = rest[rows_at[-3] : rows_at[-3] + classes, :shared]
    loss_ref[...] = rest[rows_at[-2] : rows_at[-2] + 1, : loss_ref.shape[1]]
    for piece in pieces:
        piece[1].wait()


def vmem():
    return pl.BlockSpec(memory_space=pltpu.VMEM)


def hbm():
    return pl.BlockSpec(memory_space=pltpu.HBM)


def shape(dims, kind):
    return jax.ShapeDtypeStruct(dims, kind)


def per_device(
    patches, labels, assign, patch_embed, positions, client_in, client_down,
    server_in, server_down, classifier,
):
    n = lax.axis_size("client")
    group = n // SHARDS
    rows = patches.shape[0]
    patch = patches.shape[1]
    width = client_in.shape[0]
    cols = client_in.shape[1]
    ff = client_down.shape[0]
    layers = server_in.shape[0]
    rows_in = server_in.shape[1]
    rows_down = server_down.shape[1]
    classes = classifier.shape[2]
    piece = rows // group
    halves = 2 if piece % (2 * PAD) == 0 else 1
    per_image = IMG // group
    capacity = SLOTS * group
    s_rows = capacity * piece
    r_in = cols // n
    own = width // n
    steps = bits_of(n)
    pad = pad_of(own)
    plan = chain_plan(n, r_in, ff // width, pad)
    shards = classifier.shape[0]
    rows_at = layout_of(r_in, ff // width, pad)
    per = LANES // (width // HEADS)
    spaces = [
        ((s_rows, width), BF),
        ((s_rows, 1), F32),
        ((s_rows, 3 * width), BF),
        ((s_rows // LANES * (width // LANES), per * LANES, LANES), BF),
        ((s_rows, width), BF),
        ((s_rows, width), BF),
        ((s_rows, 1), F32),
        ((s_rows, ff), BF),
        ((s_rows, ff), BF),
    ]
    scratch = [
        pltpu.SMEM((n,), jnp.int32),
        pltpu.SMEM((n * IMG,), jnp.int32),
        pltpu.VMEM((patch, rows), BF),
        pltpu.VMEM((patch, width), BF),
        pltpu.VMEM((TOK, width), BF),
        pltpu.VMEM((classes, shards, width), BF),
        pltpu.VMEM((s_rows, patch), BF),
    ]
    scratch += [pltpu.VMEM((layers + 1,) + dims, kind) for dims, kind in spaces]
    scratch += [
        pltpu.VMEM((s_rows, 3 * width), BF),
        pltpu.VMEM((s_rows, width), F32),
        pltpu.VMEM((classes, width), BF),
        pltpu.VMEM((group - 1, classes, width), BF),
        pltpu.VMEM((2, 2, plan[UPPER][0], width), BF),
        pltpu.VMEM((2, plan[UPPER][0], width), BF),
    ]
    for dims in ((group,), (PLANE, group), (PLANE, capacity), (PLANE, capacity)):
        scratch += [pltpu.VMEM(dims + (piece // halves, patch), BF)] * halves
    scratch += [pltpu.VMEM((width, cols), BF)] * (layers + 1)
    scratch += [pltpu.VMEM((ff, width), BF)] * (layers + 1)
    scratch += [pltpu.VMEM((width, cols), BF)] * layers
    scratch += [pltpu.VMEM((ff, width), BF)] * layers
    scratch += [pltpu.VMEM((group - 1, rows_in, cols), BF)] * layers
    scratch += [pltpu.VMEM((group - 1, rows_down, width), BF)] * layers
    scratch += [pltpu.VMEM((1 << len(order), r, width), BF) for r, order in plan]
    for r, order in plan:
        count = len(order)
        scratch += [pltpu.VMEM((1 << (count - 1 - t), r, width), BF) for t in range(count)]
        scratch += [pltpu.VMEM((1 << (count - 1 - t), r, width), BF) for t in range(count - 1)]
    scratch += [
        pltpu.SemaphoreType.DMA(dims)
        for dims in [
            (8,), (layers, 2), (halves, group), (halves, group), (halves, PLANE, group),
            (halves, PLANE, group), (halves, PLANE), (halves, PLANE), (layers, group, 2), (layers, group, 2), (layers, group, 2),
            (layers, group, 2), (group,), (group,), (len(plan), steps), (len(plan), steps),
            (2,), (2,), (layers, 2),
        ]
    ]
    found = pl.pallas_call(
        functools.partial(
            step_kernel, n, group, layers, per_image, capacity, classes, plan, halves
        ),
        out_shape=[
            shape((layers, rows_in, cols), BF),
            shape((layers, rows_down, width), BF),
            shape((rows_at[-1], width), F32),
        ],
        in_specs=[hbm()] * 10,
        out_specs=[hbm(), hbm(), vmem()],
        scratch_shapes=scratch,
        compiler_params=pltpu.CompilerParams(
            collective_id=1, has_side_effects=True, vmem_limit_bytes=VMEM_LIMIT
        ),
    )(
        assign.reshape(n), labels, patches.T, patch_embed, positions,
        classifier.transpose(2, 0, 1), client_in, client_down, server_in, server_down,
    )
    cuts = 4 if rows_in % (4 * PAD) == 0 else 1
    gin, gdown, gclass, loss, cin, cdown, embed, pos = pl.pallas_call(
        functools.partial(finish_kernel, cuts, rows_at),
        out_shape=[
            shape((layers, rows_in, cols), F32),
            shape((layers, rows_down, width), F32),
            shape((classes, rows_in), F32),
            shape((1, capacity * per_image), F32),
            shape((r_in, width), F32),
            shape((own, ff), F32),
            shape((own, patch), F32),
            shape((TOK, own), F32),
        ],
        in_specs=[hbm()] * 3,
        out_specs=[hbm()] * 2 + [vmem()] * 6,
        scratch_shapes=[
            pltpu.VMEM((layers, rows_in, cols), BF),
            pltpu.VMEM((layers, rows_down, width), BF),
            pltpu.VMEM((rows_at[-1], width), F32),
            pltpu.VMEM((layers, rows_in, cols), F32),
            pltpu.VMEM((layers, rows_down, width), F32),
            pltpu.SemaphoreType.DMA((layers, cuts, 2)),
            pltpu.SemaphoreType.DMA((layers, cuts, 2)),
            pltpu.SemaphoreType.DMA,
        ],
        compiler_params=pltpu.CompilerParams(vmem_limit_bytes=67000000),
    )(*found)
    return loss, embed.T, pos, cin.T, cdown.T, gin, gdown, gclass.T


def solution(mesh):
    whole = P()
    in_specs = (
        P("client", None), whole, whole, whole, whole, whole, whole,
        P(None, "client", None), P(None, "client", None), whole,
    )
    out_specs = (
        P("client", None), P(None, "client"), P(None, "client"), P(None, "client"),
        P(None, "client"), P(None, "client", None), P(None, "client", None), P("client", None),
    )
    return jax.shard_map(
        per_device, mesh=mesh, in_specs=in_specs, out_specs=out_specs, check_vma=False
    )
```

```python
import functools
import math

import jax
import jax.numpy as jnp
from jax import lax
from jax.experimental import pallas as pl
from jax.experimental.pallas import tpu as pltpu
from jax.sharding import PartitionSpec as P

HEADS = 6
TOK = 16
IMG = 8
SHARDS = 16
SLOTS = 2
PLANE = 4
EPSILON = 1e-06
LANES = 128
PAD = 16
BF = jnp.bfloat16
F32 = jnp.float32
HIGH = lax.Precision.HIGHEST
GELU_C = math.sqrt(2.0 / math.pi)
VMEM_LIMIT = 60 * 1024 * 1024
MESH = pl.DeviceIdType.MESH


def mm(a, b, precision=None):
    return lax.dot_general(
        a, b, (((1,), (0,)), ((), ())), precision=precision, preferred_element_type=F32
    )


def mm_nt(a, b, precision=None):
    return lax.dot_general(
        a, b, (((1,), (1,)), ((), ())), precision=precision, preferred_element_type=F32
    )


def mm_tn(a, b):
    return lax.dot_general(a, b, (((0,), (0,)), ((), ())), preferred_element_type=F32)


def norm(v):
    centre = v - jnp.mean(v, axis=-1, keepdims=True)
    scale = lax.rsqrt(jnp.mean(centre * centre, axis=-1, keepdims=True) + EPSILON)
    return centre * scale, scale


def norm_back(normed, scale, grad):
    return scale * (
        grad
        - jnp.mean(grad, axis=-1, keepdims=True)
        - normed * jnp.mean(grad * normed, axis=-1, keepdims=True)
    )


def gelu_both(v):
    sq = v * v
    t = jnp.tanh(v * (GELU_C + (GELU_C * 0.044715) * sq))
    half = 0.5 + 0.5 * t
    slope = half + (0.5 * v) * (1.0 - t * t) * (GELU_C + (GELU_C * 0.134145) * sq)
    return v * half, slope


def image_mask(per):
    row = lax.broadcasted_iota(jnp.int32, (per * LANES, LANES), 0) % LANES
    col = lax.broadcasted_iota(jnp.int32, (per * LANES, LANES), 1)
    return row // TOK == col // TOK


def lane_masks(head_dim):
    lane = lax.broadcasted_iota(jnp.int32, (LANES, LANES), 1)
    return [lane // head_dim == h for h in range(LANES // head_dim)]


def stack(value, keeps):
    return jnp.concatenate([jnp.where(k, value, jnp.zeros_like(value)) for k in keeps], axis=0)


def widen(value, per):
    return jnp.concatenate(
        [value[h * LANES : (h + 1) * LANES] for h in range(per)], axis=1
    )


def attend(qkv_ref, probs_ref, att_ref, width):
    rows = qkv_ref.shape[0]
    head_dim = width // HEADS
    per = LANES // head_dim
    inside = image_mask(per)
    keeps = lane_masks(head_dim)
    for group in range(rows // LANES):
        r = slice(group * LANES, (group + 1) * LANES)
        for pair in range(width // LANES):
            lo = pair * LANES
            q = qkv_ref[r, lo : lo + LANES]
            k = qkv_ref[r, width + lo : width + lo + LANES]
            v = qkv_ref[r, 2 * width + lo : 2 * width + lo + LANES]
            s = jnp.where(inside, mm_nt(stack(q, keeps), k), -1e30)
            e = jnp.exp(s - jnp.max(s, axis=-1, keepdims=True))
            p = (e * (1.0 / jnp.sum(e, axis=-1, keepdims=True))).astype(BF)
            probs_ref[group * (width // LANES) + pair] = p
            att_ref[r, lo : lo + LANES] = mm(widen(p, per), stack(v, keeps)).astype(BF)


def attend_back(grad, qkv_ref, probs_ref, dqkv_ref, width):
    rows = qkv_ref.shape[0]
    head_dim = width // HEADS
    per = LANES // head_dim
    keeps = lane_masks(head_dim)
    for group in range(rows // LANES):
        r = slice(group * LANES, (group + 1) * LANES)
        for pair in range(width // LANES):
            lo = pair * LANES
            q = qkv_ref[r, lo : lo + LANES]
            k = qkv_ref[r, width + lo : width + lo + LANES]
            v = qkv_ref[r, 2 * width + lo : 2 * width + lo + LANES]
            go = stack(grad[r, lo : lo + LANES].astype(BF), keeps)
            p = probs_ref[group * (width // LANES) + pair]
            dp = mm_nt(go, v)
            dv = mm_tn(p, go)
            pf = p.astype(F32)
            ds = (pf * (dp - jnp.sum(pf * dp, axis=-1, keepdims=True))).astype(BF)
            dq = mm(widen(ds, per), stack(k, keeps)) * (1.0 / math.sqrt(head_dim))
            dk = mm_tn(ds, stack(q, keeps))
            dqkv_ref[r, lo : lo + LANES] = dq.astype(BF)
            dqkv_ref[r, width + lo : width + lo + LANES] = dk.astype(BF)
            dqkv_ref[r, 2 * width + lo : 2 * width + lo + LANES] = dv.astype(BF)


def block_forward(x, w_ref, d_ref, first, qkv_ref, probs_ref, att_ref, second, h_ref, slope_ref):
    width = x.shape[1]
    ff = d_ref.shape[0]
    u, scale = norm(x)
    u = u.astype(BF)
    first[0][...] = u
    first[1][...] = scale
    for part in range(3):
        value = mm(u, w_ref[:, part * width : (part + 1) * width])
        if part == 0:
            value = value * (1.0 / math.sqrt(width // HEADS))
        qkv_ref[:, part * width : (part + 1) * width] = value.astype(BF)
    attend(qkv_ref, probs_ref, att_ref, width)
    y = x + mm(att_ref[...], w_ref[:, 3 * width : 4 * width])
    u, scale = norm(y)
    u = u.astype(BF)
    second[0][...] = u
    second[1][...] = scale
    for lo in range(0, ff, width):
        value, slope = gelu_both(mm(u, w_ref[:, 4 * width + lo : 5 * width + lo]))
        h_ref[:, lo : lo + width] = value.astype(BF)
        slope_ref[:, lo : lo + width] = slope.astype(BF)
    return y + mm(h_ref[...], d_ref[...])


def block_backward(
    g, w_ref, d_ref, first, qkv_ref, probs_ref, att_ref, second, h_ref, slope_ref, dqkv_ref,
    put_in, put_down, after=lambda stage: None,
):
    width = g.shape[1]
    ff = d_ref.shape[0]
    gb = g.astype(BF)
    put_down(h_ref, gb)
    after(0)
    for lo in range(0, ff, width):
        slope = slope_ref[:, lo : lo + width].astype(F32)
        slope_ref[:, lo : lo + width] = (mm_nt(gb, d_ref[lo : lo + width, :]) * slope).astype(BF)
    put_in(4 * width, second[0], slope_ref)
    after(1)
    dy = g + norm_back(
        second[0][...].astype(F32), second[1][...], mm_nt(slope_ref[...], w_ref[:, 4 * width :])
    )
    gb = dy.astype(BF)
    dqkv_ref[:, :width] = gb
    put_in(3 * width, att_ref, dqkv_ref.at[:, :width])
    after(2)
    attend_back(
        mm_nt(gb, w_ref[:, 3 * width : 4 * width]), qkv_ref, probs_ref, dqkv_ref, width
    )
    after(3)
    put_in(0, first[0], dqkv_ref)
    after(4)
    return dy + norm_back(
        first[0][...].astype(F32), first[1][...], mm_nt(dqkv_ref[...], w_ref[:, : 3 * width])
    )


def bits_of(n):
    return n.bit_length() - 1


def place_of(device, order):
    index = 0
    for bit in order:
        index = index * 2 + (device >> bit & 1)
    return index


def pad_of(own):
    return (own + 7) // 8 * 8


def chain_plan(n, r_in, blocks, pad):
    steps = bits_of(n)
    rest = list(range(1, steps))
    far = rest[-2:]
    near = rest[:-2]
    low = near[: len(near) // 2]
    high = near[len(near) // 2 :]
    first = [0] + low + high + far
    second = [0] + high + low + far
    third = [0] + far + low + high
    top = (r_in // 2 + PAD - 1) // PAD * PAD
    return [
        (pad, first), (pad, second), ((blocks - 2) * pad, third),
        (top, first[:-1]), (r_in - top, second[:-1]),
        (top, first[:-1]), (r_in - top, second[:-1]),
        (pad, third),
    ]


DOWN, UPPER, LOWER, LAST = 0, 3, 5, 7


def layout_of(r_in, blocks, pad):
    sizes = [r_in] + [pad] * (blocks + 1) + [16, 8]
    starts = [0]
    for size in sizes:
        starts.append(starts[-1] + size)
    return starts


def step_kernel(n, group, layers, per_image, capacity, classes, plan, halves, *refs):
    (
        assign_hbm, label_hbm, turned_hbm, embed_hbm, pos_hbm, class_hbm,
        cin_hbm, cdown_hbm, sin_hbm, sdown_hbm,
    ) = refs[:10]
    refs = refs[10:]
    gin_sum, gdown_sum, rest = refs[:3]
    refs = refs[3:]
    (
        assign_ref, label_ref, turned_ref, embed_ref, pos_ref, class_ref,
        slots_ref, first_u, first_s, qkv, probs, att, second_u, second_s, hidden,
        slope, dqkv, gcur,
        gclass_own, gclass_got, joined, joined_got,
    ) = refs[:22]
    refs = refs[22:]
    patch_ref, column, refs = refs[:halves], refs[halves : 2 * halves], refs[2 * halves :]
    pack, got_slots, refs = refs[:halves], refs[halves : 2 * halves], refs[2 * halves :]
    wbuf, dbuf, refs = refs[: layers + 1], refs[layers + 1 : 2 * layers + 2], refs[2 * layers + 2 :]
    gin, gdown, refs = refs[:layers], refs[layers : 2 * layers], refs[2 * layers :]
    gin_got, gdown_got, refs = refs[:layers], refs[layers : 2 * layers], refs[2 * layers :]
    chains = len(plan)
    packs, refs = refs[:chains], refs[chains:]
    got, held = [], []
    for rows, order in plan:
        count = len(order)
        got.append(refs[:count])
        held.append(refs[count : 2 * count - 1])
        refs = refs[2 * count - 1 :]
    (
        load_sem, own_sem, near_send, near_recv, far_send, far_recv, flat_send, flat_recv,
        w_send, w_recv, g_send, g_recv, c_send, c_recv, r_send, r_recv, j_send, j_recv, o_sem,
    ) = refs
    steps = bits_of(n)
    me = lax.axis_index("client")
    rank = me % group
    shard = me // group
    line = shard // PLANE
    spot = shard % PLANE
    rows_in = sin_hbm.shape[1]
    rows_down = sdown_hbm.shape[1]
    rows, width = gcur.shape
    ff = dbuf[0].shape[0]
    rows_at = layout_of(wbuf[0].shape[1] // n, ff // width, pad_of(width // n))

    loads = [
        pltpu.make_async_copy(source, target, load_sem.at[i])
        for i, (source, target) in enumerate([
            (turned_hbm, turned_ref), (assign_hbm, assign_ref), (label_hbm, label_ref),
            (embed_hbm, embed_ref), (pos_hbm, pos_ref), (class_hbm, class_ref),
            (cin_hbm, wbuf[0]), (cdown_hbm, dbuf[0]),
        ])
    ]
    for c in loads:
        c.start()

    def own_in(layer):
        return pltpu.make_async_copy(
            sin_hbm.at[layer],
            wbuf[layer + 1].at[pl.ds(rank * rows_in, rows_in)],
            own_sem.at[layer, 0],
        )

    def own_down(layer):
        return pltpu.make_async_copy(
            sdown_hbm.at[layer],
            dbuf[layer + 1].at[pl.ds(rank * rows_down, rows_down)],
            own_sem.at[layer, 1],
        )

    def near_peer(i):
        return shard * group + lax.rem(rank + i, group)

    def far_peer(i):
        return (lax.rem(line + i, PLANE) * PLANE + spot) * group + rank

    def flat_peer(i):
        return (line * PLANE + lax.rem(spot + i, PLANE)) * group + rank

    def remote(source, target, send, recv, peer):
        return pltpu.make_async_remote_copy(
            src_ref=source, dst_ref=target, send_sem=send, recv_sem=recv,
            device_id=(peer,), device_id_type=MESH,
        )

    def near(h, i):
        to = lax.rem(rank + i, group)
        return remote(
            patch_ref[h].at[to], column[h].at[line, rank], near_send.at[h, i], near_recv.at[h, i],
            near_peer(i),
        )

    def far(h, i, j):
        if j == 0:
            source, member = patch_ref[h].at[rank], rank
        else:
            member = lax.rem(rank + group - j, group)
            source = column[h].at[line, member]
        return remote(
            source, column[h].at[line, member], far_send.at[h, i, j], far_recv.at[h, i, j],
            far_peer(i),
        )

    def flat(h, i):
        return remote(
            pack[h].at[i], got_slots[h].at[spot], flat_send.at[h, i], flat_recv.at[h, i],
            flat_peer(i),
        )

    def weight_in(layer, i):
        return remote(
            sin_hbm.at[layer],
            wbuf[layer + 1].at[pl.ds(rank * rows_in, rows_in)],
            w_send.at[layer, i, 0], w_recv.at[layer, i, 0], near_peer(i),
        )

    def weight_down(layer, i):
        return remote(
            sdown_hbm.at[layer],
            dbuf[layer + 1].at[pl.ds(rank * rows_down, rows_down)],
            w_send.at[layer, i, 1], w_recv.at[layer, i, 1], near_peer(i),
        )

    def grad_in(layer, i):
        to = lax.rem(rank + i, group)
        return remote(
            gin[layer].at[pl.ds(to * rows_in, rows_in)],
            gin_got[layer].at[i - 1], g_send.at[layer, i, 0], g_recv.at[layer, i, 0], near_peer(i),
        )

    def grad_down(layer, i):
        to = lax.rem(rank + i, group)
        return remote(
            gdown[layer].at[pl.ds(to * rows_down, rows_down)],
            gdown_got[layer].at[i - 1], g_send.at[layer, i, 1], g_recv.at[layer, i, 1],
            near_peer(i),
        )

    def grad_class(i):
        return remote(gclass_own, gclass_got.at[i - 1], c_send.at[i], c_recv.at[i], near_peer(i))

    barrier = pltpu.get_barrier_semaphore()
    peers = [near_peer(i) for i in range(1, group)]
    peers += [far_peer(i) for i in range(1, PLANE)]
    peers += [flat_peer(i) for i in range(1, PLANE)]
    for peer in peers:
        pl.semaphore_signal(barrier, inc=1, device_id=(peer,), device_id_type=MESH)
    for layer in range(layers):
        own_in(layer).start()
        own_down(layer).start()
    loads[0].wait()
    turned = turned_ref[...].astype(F32).T.astype(BF)
    piece = turned.shape[0] // group
    size = piece // halves
    for i in range(group):
        for h in range(halves):
            lo = i * piece + h * size
            patch_ref[h][i] = turned[lo : lo + size]
    pl.semaphore_wait(barrier, len(peers))

    for h in range(halves):
        for i in range(1, group):
            near(h, i).start()
        for i in (2, 1, 3):
            far(h, i, 0).start()
    for layer in range(layers):
        for i in range(1, group):
            weight_in(layer, i).start()
            weight_down(layer, i).start()
    for h in range(halves):
        for j in range(1, group):
            near(h, j).wait_recv()
            for i in (2, 1, 3):
                far(h, i, j).start()
        column[h][line, rank] = patch_ref[h][rank]

    targets = [line * PLANE + lax.rem(spot + i, PLANE) for i in range(PLANE)]
    loads[1].wait()
    loads[2].wait()

    def scan(c, carry):
        there = assign_ref[c]
        out = []
        for i in range(PLANE):
            count, slots = carry[i]
            hit = there == targets[i]
            slots = tuple(
                jnp.where(hit & (count == k), c, slots[k]) for k in range(capacity)
            )
            out.append((count + jnp.where(hit, 1, 0), slots))
        return tuple(out)

    zero = jnp.int32(0)
    table = lax.fori_loop(
        0, n, scan, tuple((zero, tuple(zero for _ in range(capacity))) for _ in range(PLANE))
    )
    filled, slots = table[0]
    images = capacity * per_image
    row = lax.broadcasted_iota(jnp.int32, (images, classes), 0)
    lane = lax.broadcasted_iota(jnp.int32, (images, classes), 1)
    want = jnp.full((images, classes), -1, jnp.int32)
    for k in range(capacity):
        base = slots[k] * (group * per_image) + rank * per_image
        for j in range(per_image):
            lab = jnp.where(k < filled, label_ref[base + j], -1)
            want = jnp.where(row == k * per_image + j, lab, want)
    hot = (lane == want).astype(F32)
    full = (want[:, :1] >= 0).astype(F32)
    loads[5].wait()
    every = class_ref[...].astype(F32)
    chosen = lax.broadcasted_iota(jnp.int32, every.shape, 1) == shard
    cls = jnp.sum(jnp.where(chosen, every, 0.0), axis=1).astype(BF)

    def pick(h, c):
        home = c // group
        return column[h][home // PLANE, c % group]

    for h in range(halves):
        for i in range(1, PLANE):
            for j in range(group):
                far(h, i, j).wait_recv()
        for i in (3, 1, 2):
            for k in range(capacity):
                pack[h][i, k] = pick(h, table[i][1][k])
            flat(h, i).start()
        for k in range(capacity):
            got_slots[h][spot, k] = pick(h, slots[k])
    for c in (3, 4, 6, 7):
        loads[c].wait()
    for h in range(halves):
        for i in range(1, PLANE):
            flat(h, i).wait_recv()
        for k in range(capacity):
            home = slots[k] // group
            lo = k * piece + h * size
            slots_ref[lo : lo + size, :] = got_slots[h][home % PLANE, k]

    x = mm(slots_ref[...], embed_ref[...])
    pos = pos_ref[...].astype(F32)
    gcur[...] = x + jnp.concatenate([pos] * (rows // TOK), axis=0)

    def saved(layer):
        return (
            (first_u.at[layer], first_s.at[layer]), qkv.at[layer], probs.at[layer], att.at[layer],
            (second_u.at[layer], second_s.at[layer]), hidden.at[layer], slope.at[layer],
        )

    for layer in range(layers + 1):
        if layer > 0:
            own_in(layer - 1).wait()
            own_down(layer - 1).wait()
            for i in range(1, group):
                weight_in(layer - 1, i).wait_recv()
                weight_down(layer - 1, i).wait_recv()

        out = block_forward(gcur[...], wbuf[layer], dbuf[layer], *saved(layer))
        gcur[...] = out if layer else out.astype(BF).astype(F32)

    pool = (
        lax.broadcasted_iota(jnp.int32, (images, rows), 1) // TOK
        == lax.broadcasted_iota(jnp.int32, (images, rows), 0)
    ).astype(F32) * (1.0 / TOK)
    unpool = (
        lax.broadcasted_iota(jnp.int32, (rows, images), 0) // TOK
        == lax.broadcasted_iota(jnp.int32, (rows, images), 1)
    ).astype(F32) * (1.0 / TOK)
    u, scale = norm(mm(pool, gcur[...], HIGH))
    pooled = u.astype(BF)
    logits = mm_nt(pooled, cls)
    top = jnp.max(logits, axis=-1, keepdims=True)
    e = jnp.exp(logits - top)
    total = jnp.sum(e, axis=-1, keepdims=True)
    loss = (
        jnp.log(total) + top - jnp.sum(jnp.where(lane == want, logits, 0.0), axis=-1, keepdims=True)
    ) * full
    eye = (
        lax.broadcasted_iota(jnp.int32, (images, images), 0)
        == lax.broadcasted_iota(jnp.int32, (images, images), 1)
    )
    rest[rows_at[-2] : rows_at[-2] + 1, :images] = jnp.sum(
        jnp.where(eye, loss, 0.0), axis=0, keepdims=True
    )
    dlog = ((e / total - hot) * full).astype(BF)
    gclass_own[...] = mm_tn(dlog, pooled).astype(BF)
    for i in range(1, group):
        grad_class(i).start()
    dpool = norm_back(u, scale, mm(dlog, cls))
    gcur[...] = mm(unpool, dpool, HIGH)

    for layer in reversed(range(layers)):
        def put_in(start, lhs, rhs, layer=layer):
            for c in range(0, rhs.shape[1], width):
                gin[layer][:, start + c : start + c + width] = mm_tn(
                    lhs[...], rhs[:, c : c + width]
                ).astype(BF)

        def put_down(h, gb, layer=layer):
            for c in range(0, ff, width):
                gdown[layer][c : c + width] = mm_tn(h[:, c : c + width], gb).astype(BF)

        deep = layer + 1
        gcur[...] = block_backward(
            gcur[...], wbuf[deep], dbuf[deep], *saved(deep), dqkv, put_in, put_down,
        )
        if layer:
            for i in range(1, group):
                grad_down(layer, i).start()
                grad_in(layer, i).start()

    def peer_of(bit):
        return me + (1 << bit) - 2 * (1 << bit) * (me // (1 << bit) % 2)

    def mine(bit):
        return me // (1 << bit) % 2

    def source(c, t):
        return packs[c] if t == 0 else held[c][t - 1]

    def size_at(c, t):
        return packs[c].shape[0] >> (t + 1)

    def copy(c, t):
        bit = plan[c][1][t]
        half = size_at(c, t)
        return remote(
            source(c, t).at[pl.ds((1 - mine(bit)) * half, half)], got[c][t],
            r_send.at[c, t], r_recv.at[c, t], peer_of(bit),
        )

    def join(c):
        bit = steps - 1
        take = plan[UPPER + c][0]
        return remote(
            joined.at[c, 1 - mine(bit), pl.ds(0, take)], joined_got.at[c, pl.ds(0, take)],
            j_send.at[c], j_recv.at[c], peer_of(bit),
        )

    def store_final(c, value):
        if c == LAST or c < UPPER:
            lo = rows_at[-4] if c == LAST else rows_at[1 + c]
            rest[lo : lo + value.shape[0], :] = value
        else:
            side = 1 if c < LOWER else 0
            joined[(c - UPPER) % 2, side, : value.shape[0]] = value.astype(BF)

    progress = [0] * chains

    def advance(c):
        t = progress[c]
        count = len(plan[c][1])
        if t >= count:
            return
        progress[c] = t + 1
        half = size_at(c, t)
        copy(c, t).wait_recv()
        first = mine(plan[c][1][t]) * half
        if t == count - 1:
            store_final(c, source(c, t)[first].astype(F32) + got[c][t][0].astype(F32))
            return

        def add(e, carry):
            held[c][t][e] = (
                source(c, t)[first + e].astype(F32) + got[c][t][e].astype(F32)
            ).astype(BF)
            return carry

        lax.fori_loop(0, half, add, 0)
        copy(c, t + 1).start()

    per_dev = wbuf[0].shape[1] // n
    cols = width // n
    pad = pad_of(cols)
    src = lax.broadcasted_iota(jnp.int32, (width, n * pad), 0)
    dst = lax.broadcasted_iota(jnp.int32, (width, n * pad), 1)
    spread_to = ((dst // pad == src // cols) & (dst % pad == src % cols)).astype(F32).astype(BF)
    tok = (
        lax.broadcasted_iota(jnp.int32, (rows, LANES), 0) % TOK
        == lax.broadcasted_iota(jnp.int32, (rows, LANES), 1)
    ).astype(F32).astype(BF)

    def put_in(start, lhs, rhs):
        base = UPPER if start >= 4 * width else LOWER
        for c in range(0, rhs.shape[1], width):
            part = mm_tn(rhs[:, c : c + width], lhs[...]).astype(BF)
            first = (start + c) // per_dev
            for j in range(width // per_dev):
                lo = j * per_dev
                for piece_at in range(2):
                    take, order = plan[base + piece_at]
                    packs[base + piece_at][place_of(first + j, order)] = part[lo : lo + take]
                    lo += take

    def put_down(h, gb):
        spread = mm(gb, spread_to).astype(BF)
        for q in range(ff // width):
            part = mm_tn(spread, h[:, q * width : (q + 1) * width]).astype(BF)
            c = DOWN + min(q, 2)
            lo = max(q - 2, 0) * pad
            for j in range(n):
                packs[c][place_of(j, plan[c][1]), lo : lo + pad] = part[j * pad : (j + 1) * pad]

    def after(stage):
        if stage == 0:
            for c in range(DOWN, UPPER):
                copy(c, 0).start()
        elif stage == 1:
            for c in range(UPPER, LOWER):
                copy(c, 0).start()
        elif stage == 2:
            for c in (DOWN + 2, DOWN, DOWN + 1):
                advance(c)
        elif stage == 3:
            for c in range(UPPER, LOWER):
                advance(c)
        elif stage == 4:
            for c in range(LOWER, LAST):
                copy(c, 0).start()
            for i in range(1, group):
                grad_down(0, i).start()
                grad_in(0, i).start()

    dx = block_backward(
        gcur[...].astype(BF).astype(F32), wbuf[0], dbuf[0], *saved(0), dqkv,
        put_in, put_down, after,
    )
    for c in range(LOWER, LAST):
        advance(c)
    spread = mm(dx.astype(BF), spread_to).astype(BF)
    patch = slots_ref.shape[1]
    embed_part = mm_tn(spread, slots_ref[...]).astype(BF)
    pos_part = mm_tn(spread, tok).astype(BF)
    for j in range(n):
        at = place_of(j, plan[LAST][1])
        packs[LAST][at, :, :patch] = embed_part[j * pad : (j + 1) * pad]
        packs[LAST][at, :, patch : width - LANES] = jnp.zeros((pad, width - LANES - patch), BF)
        packs[LAST][at, :, width - LANES :] = pos_part[j * pad : (j + 1) * pad]
    copy(LAST, 0).start()

    def gin_out(layer):
        return pltpu.make_async_copy(gin_got[layer].at[0], gin_sum.at[layer], o_sem.at[layer, 0])

    def gdown_out(layer):
        return pltpu.make_async_copy(
            gdown_got[layer].at[0], gdown_sum.at[layer], o_sem.at[layer, 1]
        )

    def add_layer(layer):
        for i in range(1, group):
            grad_down(layer, i).wait_recv()
            grad_in(layer, i).wait_recv()
        start = rank * rows_in
        whole = gin[layer][pl.ds(start, rows_in)].astype(F32)
        for i in range(1, group):
            whole = whole + gin_got[layer][i - 1].astype(F32)
        gin_got[layer][0] = whole.astype(BF)
        gin_out(layer).start()
        start = rank * rows_down
        whole = gdown[layer][pl.ds(start, rows_down)].astype(F32)
        for i in range(1, group):
            whole = whole + gdown_got[layer][i - 1].astype(F32)
        gdown_got[layer][0] = whole.astype(BF)
        gdown_out(layer).start()

    def finished(c):
        return progress[c] == len(plan[c][1])

    rounds = 0
    started = [False, False]
    while not all(finished(c) for c in range(chains)):
        for c in (2, 0, 1, UPPER, UPPER + 1, LAST, LOWER, LOWER + 1):
            advance(c)
            for k in range(2):
                if finished(UPPER + k) and finished(LOWER + k) and not started[k]:
                    started[k] = True
                    join(k).start()
        if rounds < layers:
            add_layer(layers - 1 - rounds)
        rounds += 1
    for i in range(1, group):
        grad_class(i).wait_recv()
    both = gclass_own[...].astype(F32)
    for i in range(1, group):
        both = both + gclass_got[i - 1].astype(F32)
    kept = both[:, :rows_in]
    for i in range(1, group):
        kept = jnp.where(rank == i, both[:, i * rows_in : (i + 1) * rows_in], kept)
    rest[rows_at[-3] : rows_at[-3] + classes, :rows_in] = kept
    lo = 0
    for c in range(2):
        join(c).wait_recv()
        take = plan[UPPER + c][0]
        rest[lo : lo + take, :] = (
            joined[c, mine(steps - 1), :take].astype(F32) + joined_got[c, :take].astype(F32)
        )
        lo += take

    for h in range(halves):
        for i in range(1, group):
            near(h, i).wait_send()
        for i in range(1, PLANE):
            flat(h, i).wait_send()
            for j in range(group):
                far(h, i, j).wait_send()
    for i in range(1, group):
        grad_class(i).wait_send()
        for layer in range(layers):
            weight_in(layer, i).wait_send()
            weight_down(layer, i).wait_send()
            grad_in(layer, i).wait_send()
            grad_down(layer, i).wait_send()
    for c in range(chains):
        for t in range(len(plan[c][1])):
            copy(c, t).wait_send()
    for c in range(2):
        join(c).wait_send()
    for layer in range(layers):
        gin_out(layer).wait()
        gdown_out(layer).wait()


def finish_kernel(
    cuts, rows_at, gin_hbm, gdown_hbm, rest_hbm,
    gin_out, gdown_out, gclass_ref, loss_ref, cin_ref, cdown_ref, embed_ref, pos_ref,
    gin_near, gdown_near, rest, gin_wide, gdown_wide, in_sem, out_sem, rest_sem,
):
    layers, rows_in, rows_down = gin_hbm.shape[0], gin_hbm.shape[1], gdown_hbm.shape[1]
    pieces = []
    for layer in range(layers):
        for j in range(cuts):
            for source, near, wide, out, size, kind in (
                (gin_hbm, gin_near, gin_wide, gin_out, rows_in // cuts, 0),
                (gdown_hbm, gdown_near, gdown_wide, gdown_out, rows_down // cuts, 1),
            ):
                at = (layer, pl.ds(j * size, size))
                pieces.append((
                    pltpu.make_async_copy(source.at[at], near.at[at], in_sem.at[layer, j, kind]),
                    pltpu.make_async_copy(wide.at[at], out.at[at], out_sem.at[layer, j, kind]),
                    near, wide, at,
                ))
    load = pltpu.make_async_copy(rest_hbm, rest, rest_sem)
    load.start()
    for piece in pieces:
        piece[0].start()
    for arrive, leave, near, wide, at in pieces:
        arrive.wait()
        wide[at] = near[at].astype(F32)
        leave.start()
    load.wait()
    cin_ref[...] = rest[: cin_ref.shape[0], :]
    own, width = cdown_ref.shape[0], rest.shape[1]
    for q in range(cdown_ref.shape[1] // width):
        lo = rows_at[1 + q]
        cdown_ref[:, q * width : (q + 1) * width] = rest[lo : lo + own, :]
    last = rest[rows_at[-4] : rows_at[-3], :]
    embed_ref[...] = last[:own, : embed_ref.shape[1]]
    pos_ref[...] = last[:, width - LANES :].T[:TOK, :own]
    classes, shared = gclass_ref.shape
    gclass_ref[...] = rest[rows_at[-3] : rows_at[-3] + classes, :shared]
    loss_ref[...] = rest[rows_at[-2] : rows_at[-2] + 1, : loss_ref.shape[1]]
    for piece in pieces:
        piece[1].wait()


def vmem():
    return pl.BlockSpec(memory_space=pltpu.VMEM)


def hbm():
    return pl.BlockSpec(memory_space=pltpu.HBM)


def shape(dims, kind):
    return jax.ShapeDtypeStruct(dims, kind)


def per_device(
    patches, labels, assign, patch_embed, positions, client_in, client_down,
    server_in, server_down, classifier,
):
    n = lax.axis_size("client")
    group = n // SHARDS
    rows = patches.shape[0]
    patch = patches.shape[1]
    width = client_in.shape[0]
    cols = client_in.shape[1]
    ff = client_down.shape[0]
    layers = server_in.shape[0]
    rows_in = server_in.shape[1]
    rows_down = server_down.shape[1]
    classes = classifier.shape[2]
    piece = rows // group
    halves = 2 if piece % (2 * PAD) == 0 else 1
    per_image = IMG // group
    capacity = SLOTS * group
    s_rows = capacity * piece
    r_in = cols // n
    own = width // n
    steps = bits_of(n)
    pad = pad_of(own)
    plan = chain_plan(n, r_in, ff // width, pad)
    shards = classifier.shape[0]
    rows_at = layout_of(r_in, ff // width, pad)
    per = LANES // (width // HEADS)
    spaces = [
        ((s_rows, width), BF),
        ((s_rows, 1), F32),
        ((s_rows, 3 * width), BF),
        ((s_rows // LANES * (width // LANES), per * LANES, LANES), BF),
        ((s_rows, width), BF),
        ((s_rows, width), BF),
        ((s_rows, 1), F32),
        ((s_rows, ff), BF),
        ((s_rows, ff), BF),
    ]
    scratch = [
        pltpu.SMEM((n,), jnp.int32),
        pltpu.SMEM((n * IMG,), jnp.int32),
        pltpu.VMEM((patch, rows), BF),
        pltpu.VMEM((patch, width), BF),
        pltpu.VMEM((TOK, width), BF),
        pltpu.VMEM((classes, shards, width), BF),
        pltpu.VMEM((s_rows, patch), BF),
    ]
    scratch += [pltpu.VMEM((layers + 1,) + dims, kind) for dims, kind in spaces]
    scratch += [
        pltpu.VMEM((s_rows, 3 * width), BF),
        pltpu.VMEM((s_rows, width), F32),
        pltpu.VMEM((classes, width), BF),
        pltpu.VMEM((group - 1, classes, width), BF),
        pltpu.VMEM((2, 2, plan[UPPER][0], width), BF),
        pltpu.VMEM((2, plan[UPPER][0], width), BF),
    ]
    for dims in ((group,), (PLANE, group), (PLANE, capacity), (PLANE, capacity)):
        scratch += [pltpu.VMEM(dims + (piece // halves, patch), BF)] * halves
    scratch += [pltpu.VMEM((width, cols), BF)] * (layers + 1)
    scratch += [pltpu.VMEM((ff, width), BF)] * (layers + 1)
    scratch += [pltpu.VMEM((width, cols), BF)] * layers
    scratch += [pltpu.VMEM((ff, width), BF)] * layers
    scratch += [pltpu.VMEM((group - 1, rows_in, cols), BF)] * layers
    scratch += [pltpu.VMEM((group - 1, rows_down, width), BF)] * layers
    scratch += [pltpu.VMEM((1 << len(order), r, width), BF) for r, order in plan]
    for r, order in plan:
        count = len(order)
        scratch += [pltpu.VMEM((1 << (count - 1 - t), r, width), BF) for t in range(count)]
        scratch += [pltpu.VMEM((1 << (count - 1 - t), r, width), BF) for t in range(count - 1)]
    scratch += [
        pltpu.SemaphoreType.DMA(dims)
        for dims in [
            (8,), (layers, 2), (halves, group), (halves, group), (halves, PLANE, group),
            (halves, PLANE, group), (halves, PLANE), (halves, PLANE), (layers, group, 2), (layers, group, 2), (layers, group, 2),
            (layers, group, 2), (group,), (group,), (len(plan), steps), (len(plan), steps),
            (2,), (2,), (layers, 2),
        ]
    ]
    found = pl.pallas_call(
        functools.partial(
            step_kernel, n, group, layers, per_image, capacity, classes, plan, halves
        ),
        out_shape=[
            shape((layers, rows_in, cols), BF),
            shape((layers, rows_down, width), BF),
            shape((rows_at[-1], width), F32),
        ],
        in_specs=[hbm()] * 10,
        out_specs=[hbm(), hbm(), vmem()],
        scratch_shapes=scratch,
        compiler_params=pltpu.CompilerParams(
            collective_id=1, has_side_effects=True, vmem_limit_bytes=VMEM_LIMIT
        ),
    )(
        assign.reshape(n), labels, patches.T, patch_embed, positions,
        classifier.transpose(2, 0, 1), client_in, client_down, server_in, server_down,
    )
    cuts = 4 if rows_in % (4 * PAD) == 0 else 1
    gin, gdown, gclass, loss, cin, cdown, embed, pos = pl.pallas_call(
        functools.partial(finish_kernel, cuts, rows_at),
        out_shape=[
            shape((layers, rows_in, cols), F32),
            shape((layers, rows_down, width), F32),
            shape((classes, rows_in), F32),
            shape((1, capacity * per_image), F32),
            shape((r_in, width), F32),
            shape((own, ff), F32),
            shape((own, patch), F32),
            shape((TOK, own), F32),
        ],
        in_specs=[hbm()] * 3,
        out_specs=[hbm()] * 2 + [vmem()] * 6,
        scratch_shapes=[
            pltpu.VMEM((layers, rows_in, cols), BF),
            pltpu.VMEM((layers, rows_down, width), BF),
            pltpu.VMEM((rows_at[-1], width), F32),
            pltpu.VMEM((layers, rows_in, cols), F32),
            pltpu.VMEM((layers, rows_down, width), F32),
            pltpu.SemaphoreType.DMA((layers, cuts, 2)),
            pltpu.SemaphoreType.DMA((layers, cuts, 2)),
            pltpu.SemaphoreType.DMA,
        ],
        compiler_params=pltpu.CompilerParams(vmem_limit_bytes=67000000),
    )(*found)
    return loss, embed.T, pos, cin.T, cdown.T, gin, gdown, gclass.T


def solution(mesh):
    whole = P()
    in_specs = (
        P("client", None), whole, whole, whole, whole, whole, whole,
        P(None, "client", None), P(None, "client", None), whole,
    )
    out_specs = (
        P("client", None), P(None, "client"), P(None, "client"), P(None, "client"),
        P(None, "client"), P(None, "client", None), P(None, "client", None), P("client", None),
    )
    return jax.shard_map(
        per_device, mesh=mesh, in_specs=in_specs, out_specs=out_specs, check_vma=False
    )
```
